128 devices in a mesh: rows: 32 (over z, y, core), cols: 4 (over x).
Axes of the slice: x: 4, y: 4, z: 4, core: 2. Of those that a mesh axis runs over, the one named last changes fastest.
Arguments:
- features: bfloat16 [256, 512, 512], P('rows', 'cols'), may hold values from -6 to 6
- dw_weight: float32 [49, 512], replicated, may hold values from -0.875 to 0.875
- norm_gain: float32 [512], replicated, may hold values from 0.1 to 1.9
- w_up: bfloat16 [512, 2048], replicated, may hold values from -0.25 to 0.25
- w_down: bfloat16 [2048, 512], replicated, may hold values from -0.125 to 0.125
- cotangent: bfloat16 [256, 512, 512], P('rows', 'cols'), may hold values from -6 to 6
Outputs:
- grad_input: bfloat16 [256, 512, 512], P('rows', 'cols')
- grad_dw: float32 [49, 512], replicated
- grad_gain: float32 [512], replicated
- grad_up: float32 [512, 2048], replicated
- grad_down: float32 [2048, 512], replicated
The draws below stay inside these ranges and needn't reach their ends.
All inputs are finite; a program needn't handle non-finite values.
Results may differ from the reference program's by a relative error of at most 0.019.
Values may be sent and summed in bfloat16 or wider, within the bound.
A program may use at most 128 MiB of HBM per device.

```python
import jax
import jax.numpy as jnp
from jax import lax

C = 512
FF = 2048
KK = 49
H = 256
W = 512


def shard_levels(stream_key, shape, split, smallest, largest):
    level, own = 1.0, jax.random.fold_in(stream_key, 6)
    for dim, parts in split:
        steps = jnp.exp(jax.random.uniform(jax.random.fold_in(own, dim), (parts,), jnp.float32, smallest / len(split), largest / len(split)))
        level = level * jnp.repeat(steps, shape[dim] // parts).reshape([-1 if axis == dim else 1 for axis in range(len(shape))])
    return level


def normal_values(rng, dims, scale, bound, split=(), kind=jnp.bfloat16):
    values = jax.random.normal(rng, dims, jnp.float32) * scale
    if len(split) > 0:
        values = shard_levels(rng, dims, split, -0.22, 0.18) * values
    return jnp.clip(values, min=-bound, max=bound).astype(kind)


def setup_inputs(seed: int = 0) -> dict:
    keys = jax.random.split(jax.random.key(seed), 7)
    features = normal_values(keys[0], (H, W, C), 1.0, 6.0, ((0, 32), (1, 4)))
    dw_weight = normal_values(keys[1], (KK, C), KK ** -0.5, 0.875, (), jnp.float32)
    norm_gain = jnp.clip(1.0 + 0.18 * jax.random.normal(keys[2], (C,), jnp.float32), 0.1, 1.9)
    w_up = normal_values(keys[3], (C, FF), C ** -0.5, 0.25)
    w_down = normal_values(keys[4], (FF, C), FF ** -0.5, 0.125)
    cotangent = normal_values(keys[5], (H, W, C), 1.0, 6.0, ((0, 32), (1, 4)))
    return {"features": features, "dw_weight": dw_weight, "norm_gain": norm_gain, "w_up": w_up, "w_down": w_down, "cotangent": cotangent}


eps = 1e-06

def depthwise(padded, weight, rows, cols):
    total = jnp.zeros((rows, cols, padded.shape[2]), jnp.float32)
    for tap_i in range(7):
        for tap_j in range(7):
            total = total + padded[tap_i:tap_i + rows, tap_j:tap_j + cols] * weight[7 * tap_i + tap_j]
    return total

def pointwise(conv, gain, w_up, w_down, grad_out):
    mean = lax.optimization_barrier(jnp.mean(conv, axis=-1, keepdims=True))
    centred = conv - mean
    inv = lax.rsqrt(lax.optimization_barrier(jnp.mean(centred * centred, axis=-1, keepdims=True)) + eps)
    normed = centred * inv
    scaled = (normed * gain).astype(jnp.bfloat16)
    hidden = jnp.dot(scaled, w_up, preferred_element_type=jnp.float32)
    act = (0.5 * hidden * (1.0 + lax.erf(hidden * 0.7071067811865476))).astype(jnp.bfloat16)
    grad_down = lax.dot_general(act, grad_out, (((0,), (0,)), ((), ())), preferred_element_type=jnp.float32)
    grad_act = lax.dot_general(grad_out, w_down, (((1,), (1,)), ((), ())), preferred_element_type=jnp.float32)
    slope = 0.5 * (1.0 + lax.erf(hidden * 0.7071067811865476)) + hidden * jnp.exp(-0.5 * hidden * hidden) * 0.3989422804014327
    grad_hidden = (grad_act * slope).astype(jnp.bfloat16)
    grad_up = lax.dot_general(scaled, grad_hidden, (((0,), (0,)), ((), ())), preferred_element_type=jnp.float32)
    grad_scaled = lax.dot_general(grad_hidden, w_up, (((1,), (1,)), ((), ())), preferred_element_type=jnp.float32)
    grad_gain = lax.optimization_barrier(jnp.sum(grad_scaled * normed, axis=0))
    g_norm = grad_scaled * gain
    grad_conv = inv * (g_norm - lax.optimization_barrier(jnp.mean(g_norm, axis=-1, keepdims=True)) - normed * lax.optimization_barrier(jnp.mean(g_norm * normed, axis=-1, keepdims=True)))
    return (grad_conv.astype(jnp.bfloat16), grad_up, grad_down, grad_gain)

def reference(features, dw_weight, norm_gain, w_up, w_down, cotangent):
    padded = jnp.pad(features.astype(jnp.float32), ((3, 3), (3, 3), (0, 0)))
    conv = depthwise(padded, dw_weight, H, W)
    blocks = H // 8
    conv_blocks = conv.reshape(blocks, 8 * W, C)
    grad_blocks = cotangent.reshape(blocks, 8 * W, C)

    def step(carry, pair):
        grad_conv, grad_up, grad_down, grad_gain = pointwise(pair[0], norm_gain, w_up, w_down, pair[1])
        return ((carry[0] + grad_up, carry[1] + grad_down, carry[2] + grad_gain), grad_conv)
    start = (jnp.zeros((C, FF), jnp.float32), jnp.zeros((FF, C), jnp.float32), jnp.zeros((C,), jnp.float32))
    sums, grad_conv = lax.scan(step, start, (conv_blocks, grad_blocks))
    grad_conv = grad_conv.reshape(H, W, C)
    grad_f = grad_conv.astype(jnp.float32)
    taps = []
    for tap_i in range(7):
        for tap_j in range(7):
            taps.append(lax.optimization_barrier(jnp.sum(padded[tap_i:tap_i + H, tap_j:tap_j + W] * grad_f, axis=(0, 1))))
    grad_dw = jnp.stack(taps)
    grad_pad = jnp.pad(grad_f, ((3, 3), (3, 3), (0, 0)))
    total = cotangent.astype(jnp.float32)
    for tap_i in range(7):
        for tap_j in range(7):
            total = total + grad_pad[6 - tap_i:6 - tap_i + H, 6 - tap_j:6 - tap_j + W] * dw_weight[7 * tap_i + tap_j]
    return (total.astype(jnp.bfloat16), grad_dw, sums[2], sums[0], sums[1])
```

```python
import jax
import jax.numpy as jnp
from jax import lax
from jax.experimental import pallas as pl
from jax.experimental.pallas import tpu as pltpu
from jax.sharding import PartitionSpec as P

EPS = 1e-06
ROWS, COLS, CH, FF = 8, 128, 512, 2048
PIX = ROWS * COLS
NCH = 4
FC = FF // NCH
LEFT = 8
F32, BF16 = jnp.float32, jnp.bfloat16
MESH = pl.DeviceIdType.MESH
FIRST_AXIS = ((0, 2), (1, 0), (2, 1), (0, 2))
SIDES = ((-1, 0), (1, 0), (0, -1), (0, 1), (-1, -1), (-1, 1), (1, -1), (1, 1))
(R_CORE, R_A0, R_A1, R_B0, R_B1, R_PRS, R_PAG, R_G0, R_G1, R_H0, R_H1, R_CAG) = range(12)


def kernel(
    feat_hbm, dww_hbm, gain_hbm, wup_hbm, wdn_hbm, cot_hbm,
    gin_hbm, small_hbm, big_hbm,
    fbuf, cbuf, wup, wdn, dww, gainb, xf, gp, wb, cv, invb, sc, act, gh, gs, G, gb, obuf,
    scol, hrow, hcol, hcor,
    csend, crecv, M, axa, axs, axb, pls, plr, GA, GB,
    gd, dsm, drc, dps, dpr, dax, dga, dout,
    ld, hsend, hrecv, csem, rsem, ssend, srecv, osem,
):
    ra, ca = lax.axis_index("rows"), lax.axis_index("cols")
    core = ra % 2
    y, z, x = (ra // 2) % 4, ra // 8, ca

    def device(x_, y_, z_, core_):
        return ((z_ * 4 + y_) * 2 + core_, x_)

    partner = device(x, y, z, 1 - core)

    def side(dr, dc):
        return ((ra + dr + 32) % 32, (ca + dc + 4) % 4)

    def plane_peer(d, axis):
        ix, iy, iz = axis
        u, v = ix * y + iy * z + iz * x, ix * z + iy * x + iz * y
        u2, v2 = (u + d // 4) % 4, (v + d % 4) % 4
        return (
            device(
                ix * x + iy * v2 + iz * u2,
                ix * u2 + iy * y + iz * v2,
                ix * v2 + iy * u2 + iz * z,
                core,
            ),
            u2 * 4 + v2,
        )

    def plane_pos(axis):
        ix, iy, iz = axis
        return (ix * y + iy * z + iz * x) * 4 + ix * z + iy * x + iz * y

    def axis_of(c):
        a0, a1 = FIRST_AXIS[c]
        return tuple((a0 == n) * (1 - core) + (a1 == n) * core for n in range(3))

    def along(axis, step):
        ix, iy, iz = axis
        return device(
            (x + step * ix) % 4, (y + step * iy) % 4, (z + step * iz) % 4, core
        )

    def remote(src, dst, send, recv, to):
        return pltpu.make_async_remote_copy(
            src_ref=src, dst_ref=dst, send_sem=send, recv_sem=recv, device_id=to, device_id_type=MESH
        )

    def landed(ref, sem):
        pltpu.make_async_copy(ref, ref, sem).wait()

    loads = [
        pltpu.make_async_copy(s, d, ld.at[n])
        for n, (s, d) in enumerate(
            ((feat_hbm, fbuf), (dww_hbm, dww), (gain_hbm, gainb), (cot_hbm, cbuf), (wup_hbm, wup), (wdn_hbm, wdn))
        )
    ]
    for c_ in loads:
        c_.start()
    barrier = pltpu.get_barrier_semaphore()
    pl.semaphore_signal(barrier, inc=1, device_id=partner, device_id_type=MESH)
    for dr, dc in SIDES:
        pl.semaphore_signal(barrier, inc=1, device_id=side(dr, dc), device_id_type=MESH)
    for axis in ((1, 0, 0), (0, 1, 0), (0, 0, 1)):
        @pl.loop(1, 16)
        def _(d, axis=axis):
            pl.semaphore_signal(barrier, inc=1, device_id=plane_peer(d, axis)[0], device_id_type=MESH)

    for c_ in loads[:3]:
        c_.wait()

    def edges(pad, phase):
        for n, start in ((0, LEFT), (1, LEFT + COLS - 8)):
            for cc in range(4):
                scol[phase, n, :, :, cc * 128 : cc * 128 + 128] = pad[
                    cc, 3 : 3 + ROWS, start : start + 8, :
                ].astype(BF16)

    @pl.loop(0, ROWS)
    def _(r):
        for cc in range(4):
            xf[cc, 3 + r, LEFT : LEFT + COLS, :] = fbuf[r, :, cc * 128 : cc * 128 + 128].astype(F32)

    edges(xf, 0)
    pl.semaphore_wait(barrier, 1 + len(SIDES) + 45)

    def halo_copies(phase, rows_src):
        out = []
        for n, (dr, dc) in enumerate(SIDES):
            rs = slice(0, 3) if dr < 0 else slice(5, 8)
            if dc == 0:
                src, dst = rows_src.at[rs], hrow.at[phase, n]
            elif dr == 0:
                src, dst = scol.at[phase, n - 2], hcol.at[phase, n - 2]
            else:
                src, dst = scol.at[phase, 0 if dc < 0 else 1, rs], hcor.at[phase, n - 4]
            out.append(remote(src, dst, hsend.at[phase, n], hrecv.at[phase, n], side(dr, dc)))
        return out

    valid = {
        -1: jnp.where(ra < 31, 1.0, 0.0).astype(F32),
        1: jnp.where(ra > 0, 1.0, 0.0).astype(F32),
    }
    valid_c = {
        -1: jnp.where(ca < 3, 1.0, 0.0).astype(F32),
        1: jnp.where(ca > 0, 1.0, 0.0).astype(F32),
    }

    def halo_cols(phase, copies, pad):
        for n in (2, 3):
            copies[n].wait_recv()
            dc = SIDES[n][1]
            start = LEFT + COLS if dc < 0 else LEFT - 8
            for cc in range(4):
                pad[cc, 3 : 3 + ROWS, start : start + 8, :] = (
                    hcol[phase, n - 2, :, :, cc * 128 : cc * 128 + 128].astype(F32) * valid_c[dc]
                )

    def halo_rows(phase, copies, pad):
        for n in (0, 1):
            copies[n].wait_recv()
            dr = SIDES[n][0]
            r0 = 3 + ROWS if dr < 0 else 0
            for r in range(3):
                for cc in range(4):
                    pad[cc, r0 + r, LEFT : LEFT + COLS, :] = (
                        hrow[phase, n, r, :, cc * 128 : cc * 128 + 128].astype(F32) * valid[dr]
                    )
        for n in range(4, 8):
            copies[n].wait_recv()
            dr, dc = SIDES[n]
            r0 = 3 + ROWS if dr < 0 else 0
            start = LEFT + COLS if dc < 0 else LEFT - 8
            for cc in range(4):
                pad[cc, r0 : r0 + 3, start : start + 8, :] = hcor[
                    phase, n - 4, :, :, cc * 128 : cc * 128 + 128
                ].astype(F32) * (valid[dr] * valid_c[dc])

    def conv(pad, flip, cc, cb, inner):
        rhos = range(3, 11) if inner else (0, 1, 2, 11, 12, 13)
        rows = range(ROWS) if inner else (0, 1, 2, 5, 6, 7)
        base = cb * 32

        def at(r, b):
            return pl.ds(pl.multiple_of(r * COLS + base + 8 * b, 8), 8)

        def body(j, acc):
            acc = dict(zip([(r, b) for r in rows for b in range(4)], acc))
            w = [wb[cc, (48 - 7 * i - j) if flip else (7 * i + j)] for i in range(7)]
            for rho in rhos:
                for b in range(4):
                    v = pad[cc, rho, pl.ds(base + (8 * b + LEFT - 3) + j, 8), :]
                    for r in rows:
                        if 0 <= rho - r <= 6:
                            acc[r, b] = acc[r, b] + v * w[rho - r]
            return tuple(acc.values())

        if inner:
            start = tuple(jnp.zeros((8, 128), F32) for r in rows for b in range(4))
        else:
            start = tuple(cv[cc, at(r, b), :] for r in rows for b in range(4))
        acc = lax.fori_loop(0, 7, body, start)
        for n, (r, b) in enumerate([(r, b) for r in rows for b in range(4)]):
            cv[cc, at(r, b), :] = acc[n]

    halo = halo_copies(0, fbuf)
    for n in (2, 3, 0, 1, 4, 5, 6, 7):
        halo[n].start()

    for t in range(49):
        for cc in range(4):
            wb[cc, t] = jnp.broadcast_to(dww[t : t + 1, cc * 128 : cc * 128 + 128], (8, 128))

    @pl.loop(0, 8)
    def _(t):
        conv(xf, False, t // 2, 1 + t % 2, True)

    halo_cols(0, halo, xf)

    @pl.loop(0, 8)
    def _(t):
        conv(xf, False, t // 2, 3 * (t % 2), True)

    halo_rows(0, halo, xf)

    @pl.loop(0, 16)
    def _(t):
        conv(xf, False, t // 4, t % 4, False)

    @pl.loop(0, 16)
    def _(t):
        ps = pl.ds(pl.multiple_of(t * 64, 64), 64)
        v = [cv[cc, ps, :] for cc in range(4)]
        mean = jnp.sum(v[0] + v[1] + v[2] + v[3], axis=1, keepdims=True) * (1.0 / CH)
        v = [a - mean for a in v]
        sq = [a * a for a in v]
        inv = lax.rsqrt(jnp.sum(sq[0] + sq[1] + sq[2] + sq[3], axis=1, keepdims=True) * (1.0 / CH) + EPS)
        invb[ps, :] = jnp.broadcast_to(inv, (64, 128))
        for cc in range(4):
            n_ = v[cc] * inv
            cv[cc, ps, :] = n_
            sc[ps, cc * 128 : cc * 128 + 128] = (n_ * gainb[:, cc * 128 : cc * 128 + 128]).astype(BF16)

    for c_ in loads[3:]:
        c_.wait()

    def mlp_a(c, half):
        for pb in (2 * half, 2 * half + 1):
            ps = slice(pb * 256, pb * 256 + 256)
            h = jnp.dot(sc[ps, :], wup[:, c * FC : (c + 1) * FC], preferred_element_type=F32)
            ga = lax.dot_general(
                cbuf[ps, :], wdn[c * FC : (c + 1) * FC, :], (((1,), (1,)), ((), ())), preferred_element_type=F32
            )
            phi = 0.5 * (1.0 + lax.erf(h * 0.7071067811865476))
            act[ps, :] = (h * phi).astype(BF16)
            e = jnp.exp(-0.5 * h * h) * 0.3989422804014327
            gh[ps, :] = (ga * (phi + h * e)).astype(BF16)

    def put(c, slot, value):
        G[c, slot, 0] = value[:, 0:256]
        G[c, slot, 1] = value[:, 256:512]

    def mlp_down(c):
        put(c, core, lax.dot_general(act[...], cbuf[...], (((0,), (0,)), ((), ())), preferred_element_type=F32))

    def mlp_up(c):
        put(c, 1 - core, lax.dot_general(sc[...], gh[...], (((0,), (0,)), ((), ())), preferred_element_type=F32))

    def mlp_back(c):
        v = lax.dot_general(
            gh[...], wup[:, c * FC : (c + 1) * FC], (((1,), (1,)), ((), ())), preferred_element_type=F32
        )
        gs[...] = v if c == 0 else gs[...] + v

    def blocks(fn):
        @pl.loop(0, 8)
        def _(t):
            fn(t // 2, pl.ds((t % 2) * 8, 8), t)

    def st0(c):
        def go(a, n, t):
            rows = pl.ds(pl.multiple_of((t % 4) * 128, 128), 128)
            csend[c, a, n] = G[c, 1, t // 4, rows, :].reshape(8, 16, 256).astype(BF16)
        blocks(go)
        remote(csend.at[c], crecv.at[c], csem.at[c, R_CORE], rsem.at[c, R_CORE], partner).start()

    def st1(c):
        landed(crecv.at[c], rsem.at[c, R_CORE])
        axis = axis_of(c)
        p = axis[0] * x + axis[1] * y + axis[2] * z
        def go(a, n, t):
            rows = pl.ds(pl.multiple_of((t % 4) * 128, 128), 128)
            M[c, a, n] = (
                G[c, 0, t // 4, rows, :].reshape(8, 16, 256) + crecv[c, a, n].astype(F32)
            ).astype(BF16)
        blocks(go)
        far = (p + 2) % 4
        remote(M.at[c, far, 0:8], axa.at[c, 0], csem.at[c, R_A0], rsem.at[c, R_A0], along(axis, 1)).start()
        remote(M.at[c, far, 8:16], axa.at[c, 1], csem.at[c, R_A1], rsem.at[c, R_A1], along(axis, 3)).start()

    def st2(c):
        axis = axis_of(c)
        p = axis[0] * x + axis[1] * y + axis[2] * z
        landed(axa.at[c, 0], rsem.at[c, R_A0])
        landed(axa.at[c, 1], rsem.at[c, R_A1])
        right, left = (p + 1) % 4, (p + 3) % 4
        axs[c, 0, 0:8] = (M[c, right, 0:8].astype(F32) + axa[c, 0].astype(F32)).astype(BF16)
        axs[c, 0, 8:16] = M[c, right, 8:16]
        remote(axs.at[c, 0], axb.at[c, 0], csem.at[c, R_B0], rsem.at[c, R_B0], along(axis, 1)).start()
        axs[c, 1, 0:8] = M[c, left, 0:8]
        axs[c, 1, 8:16] = (M[c, left, 8:16].astype(F32) + axa[c, 1].astype(F32)).astype(BF16)
        remote(axs.at[c, 1], axb.at[c, 1], csem.at[c, R_B1], rsem.at[c, R_B1], along(axis, 3)).start()

    def st3(c):
        axis = axis_of(c)
        p = axis[0] * x + axis[1] * y + axis[2] * z
        landed(axb.at[c, 0], rsem.at[c, R_B0])
        landed(axb.at[c, 1], rsem.at[c, R_B1])
        pls[c] = (M[c, p].astype(F32) + axb[c, 0].astype(F32) + axb[c, 1].astype(F32)).astype(BF16)

        @pl.loop(1, 16)
        def _(d):
            to, pos = plane_peer(d, axis)
            remote(pls.at[c, pos], plr.at[c, d - 1], csem.at[c, R_PRS], rsem.at[c, R_PRS], to).start()

    def st4(c):
        axis = axis_of(c)
        p = axis[0] * x + axis[1] * y + axis[2] * z
        pos = plane_pos(axis)
        landed(plr.at[c], rsem.at[c, R_PRS])
        total = pls[c, pos].astype(F32)
        for d in range(15):
            total = total + plr[c, d].astype(F32)
        GA[c, p, pos] = total.astype(BF16)

        @pl.loop(1, 16)
        def _(d):
            to, _ = plane_peer(d, axis)
            remote(GA.at[c, p, pos], GA.at[c, p, pos], csem.at[c, R_PAG], rsem.at[c, R_PAG], to).start()

    def st5(c):
        axis = axis_of(c)
        p = axis[0] * x + axis[1] * y + axis[2] * z
        landed(plr.at[c], rsem.at[c, R_PAG])
        remote(GA.at[c, p], GA.at[c, p], csem.at[c, R_G0], rsem.at[c, R_G0], along(axis, 1)).start()
        remote(GA.at[c, p], GA.at[c, p], csem.at[c, R_G1], rsem.at[c, R_G1], along(axis, 3)).start()

    def st6(c):
        axis = axis_of(c)
        p = axis[0] * x + axis[1] * y + axis[2] * z
        right, left = (p + 1) % 4, (p + 3) % 4
        landed(GA.at[c, left], rsem.at[c, R_G0])
        landed(GA.at[c, right], rsem.at[c, R_G1])
        a = GA.at[c, left, 0:8]
        b = GA.at[c, right, 8:16]
        remote(a, a, csem.at[c, R_H0], rsem.at[c, R_H0], along(axis, 1)).start()
        remote(b, b, csem.at[c, R_H1], rsem.at[c, R_H1], along(axis, 3)).start()

    def st7(c):
        landed(axa.at[c, 0], rsem.at[c, R_H0])
        landed(axa.at[c, 1], rsem.at[c, R_H1])
        remote(GA.at[c], GB.at[c], csem.at[c, R_CAG], rsem.at[c, R_CAG], partner).start()
        pltpu.make_async_copy(GA.at[c], big_hbm.at[core, c], osem.at[2 * c]).start()

    def st8(c):
        landed(GB.at[c], rsem.at[c, R_CAG])
        pltpu.make_async_copy(GB.at[c], big_hbm.at[1 - core, c], osem.at[2 * c + 1]).start()

    def ln_back(quarter):
        def body(t, part):
            ps = pl.ds(pl.multiple_of(quarter * 256 + t * 64, 64), 64)
            inv = invb[ps, :]
            nv = [cv[cc, ps, :] for cc in range(4)]
            gv = [gs[ps, cc * 128 : cc * 128 + 128] for cc in range(4)]
            prod = [g * n for g, n in zip(gv, nv)]
            part = tuple(
                q + jnp.sum(pr.reshape(8, 8, 128), axis=0) for q, pr in zip(part, prod)
            )
            gains = [gainb[:, cc * 128 : cc * 128 + 128] for cc in range(4)]
            gn = [g * k for g, k in zip(gv, gains)]
            gm = [pr * k for pr, k in zip(prod, gains)]
            m1 = jnp.sum(gn[0] + gn[1] + gn[2] + gn[3], axis=1, keepdims=True) * (1.0 / CH)
            m2 = jnp.sum(gm[0] + gm[1] + gm[2] + gm[3], axis=1, keepdims=True) * (1.0 / CH)
            r, c0 = 2 * quarter + t // 2, (t % 2) * 64
            for cc in range(4):
                g = (inv * (gn[cc] - m1 - nv[cc] * m2)).astype(BF16)
                gb[r, pl.ds(pl.multiple_of(c0, 64), 64), cc * 128 : cc * 128 + 128] = g
                gp[cc, 3 + r, pl.ds(pl.multiple_of(LEFT + c0, 8), 64), :] = g.astype(F32)
            return part

        part = lax.fori_loop(0, 4, body, tuple(jnp.zeros((8, 128), F32) for _ in range(4)))
        for cc in range(4):
            row = jnp.sum(part[cc], axis=0, keepdims=True)
            gd[cc, 49:50, :] = row if quarter == 0 else gd[cc, 49:50, :] + row

    back = halo_copies(1, gb)

    def send_back():
        edges(gp, 1)
        for n in (0, 1, 2, 3, 4, 5, 6, 7):
            back[n].start()

    def gdw(cc, js):
        @pl.loop(js[0], js[1])
        def _(j):
            def body(cb, acc):
                acc = list(acc)
                base = cb * 64
                for b in range(8):
                    gv = [gp[cc, 3 + r, pl.ds(pl.multiple_of(base + LEFT + 8 * b, 8), 8), :] for r in range(8)]
                    for rho in range(14):
                        v = xf[cc, rho, pl.ds(base + (8 * b + LEFT - 3) + j, 8), :]
                        for r in range(max(0, rho - 6), min(8, rho + 1)):
                            acc[rho - r] = acc[rho - r] + v * gv[r]
                return tuple(acc)

            acc = lax.fori_loop(0, 2, body, tuple(jnp.zeros((8, 128), F32) for _ in range(7)))
            for i in range(7):
                gd[cc, pl.ds(7 * i + j, 1), :] = jnp.sum(acc[i], axis=0, keepdims=True)

    zaxis = (0, 0, 1)
    zpos = plane_pos(zaxis)

    def sm0():
        for cc in range(4):
            for tb in range(4):
                dsm[4 * cc + tb] = gd[cc, 16 * tb : 16 * tb + 16, :]
        remote(dsm, drc, ssend.at[0], srecv.at[0], partner).start()

    def sm1():
        landed(drc, srecv.at[0])
        dps[...] = dsm[...] + drc[...]

        @pl.loop(1, 16)
        def _(d):
            to, pos = plane_peer(d, zaxis)
            remote(dps.at[pos], dpr.at[d - 1], ssend.at[1], srecv.at[1], to).start()

    def sm2():
        landed(dpr, srecv.at[1])
        total = dps[zpos]
        for d in range(15):
            total = total + dpr[d]
        dax[z] = total
        for step in (1, 2, 3):
            remote(dax.at[z], dax.at[z], ssend.at[2], srecv.at[2], along(zaxis, step)).start()

    def sm3():
        landed(dpr.at[0:3], srecv.at[2])
        dga[zpos] = dax[0] + dax[1] + dax[2] + dax[3]

        @pl.loop(1, 16)
        def _(d):
            to, _ = plane_peer(d, zaxis)
            remote(dga.at[zpos], dga.at[zpos], ssend.at[3], srecv.at[3], to).start()

    def sm4():
        landed(dpr, srecv.at[3])
        for cc in range(4):
            for tb in range(4):
                dout[16 * tb : 16 * tb + 16, cc * 128 : cc * 128 + 128] = dga[4 * cc + tb]
        pltpu.make_async_copy(dout, small_hbm, osem.at[8]).start()

    def gin_inner(part, pair):
        @pl.loop(0, 4)
        def _(t):
            conv(gp, True, t, (1 + part) if pair == 0 else 3 * part, True)

    def gin_outer(cb):
        @pl.loop(0, 4)
        def _(t):
            conv(gp, True, t, cb, False)

    def gin_store(part):
        @pl.loop(part * 8, part * 8 + 8)
        def _(t):
            ps = pl.ds(pl.multiple_of(t * 64, 64), 64)
            for cc in range(4):
                cs = slice(cc * 128, cc * 128 + 128)
                obuf[ps, cs] = (cbuf[ps, cs].astype(F32) + cv[cc, ps, :]).astype(BF16)
        rows = slice(part * 512, part * 512 + 512)
        pltpu.make_async_copy(obuf.at[rows], gin_hbm.at[rows], osem.at[9 + part]).start()

    work = []
    chains = {}
    for c in range(NCH):
        work += [(0.75, lambda c=c: mlp_a(c, 0), None), (0.75, lambda c=c: mlp_a(c, 1), None)]
        work += [(0.62, lambda c=c: mlp_down(c), None), (0.62, lambda c=c: mlp_up(c), c)]
        work += [(0.62, lambda c=c: mlp_back(c), None)]
        chains[c] = list(
            zip((0.0, 1.8, 2.8, 4.0, 6.0, 6.0, 4.0, 2.8, 1.8), [lambda s=s, c=c: s(c) for s in (st0, st1, st2, st3, st4, st5, st6, st7, st8)])
        )
    work += [(0.4, lambda q=q: ln_back(q), None) for q in range(4)]
    work += [(0.2, send_back, None)]
    for cc in range(4):
        work += [(1.1, lambda cc=cc: gdw(cc, (0, 4)), None)]
        work += [(0.9, lambda cc=cc: gdw(cc, (4, 7)), "small" if cc == 3 else None)]
    chains["small"] = list(zip((0.0, 1.5, 6.5, 3.5, 6.5), (sm0, sm1, sm2, sm3, sm4)))
    work += [(1.7, lambda: gin_inner(0, 0), None), (1.7, lambda: gin_inner(1, 0), None)]
    work += [(0.1, lambda: halo_cols(1, back, gp), None)]
    work += [(1.7, lambda: gin_inner(0, 1), None), (1.7, lambda: gin_inner(1, 1), None)]
    work += [(0.3, lambda: halo_rows(1, back, gp), None)]
    work += [(0.55, lambda cb=cb: gin_outer(cb), None) for cb in range(4)]
    work += [(0.2, lambda: gin_store(0), None), (0.2, lambda: gin_store(1), None)]

    now = 0.0
    due = []

    def serve(limit):
        nonlocal now
        while due and (limit is None or min(due)[0] <= limit):
            when, key, n = min(due)
            due.remove((when, key, n))
            now = max(now, when) + 0.1
            chains[key][n][1]()
            if n + 1 < len(chains[key]):
                due.append((now + chains[key][n + 1][0], key, n + 1))

    for cost, fn, opens in work:
        fn()
        now += cost
        if opens is not None:
            due.append((now, 9 if opens == "small" else opens, 0))
            if opens == "small":
                chains[9] = chains["small"]
        serve(now)
    serve(None)

    for phase in (0, 1):
        for c_ in (halo, back)[phase]:
            c_.wait_send()
    for c in range(NCH):
        landed(csend.at[c], csem.at[c, R_CORE])
        landed(axa.at[c, 0], csem.at[c, R_A0])
        landed(axa.at[c, 1], csem.at[c, R_A1])
        landed(axb.at[c, 0], csem.at[c, R_B0])
        landed(axb.at[c, 1], csem.at[c, R_B1])
        landed(plr.at[c], csem.at[c, R_PRS])
        landed(plr.at[c], csem.at[c, R_PAG])
        landed(axb.at[c, 0], csem.at[c, R_G0])
        landed(axb.at[c, 1], csem.at[c, R_G1])
        landed(axa.at[c, 0], csem.at[c, R_H0])
        landed(axa.at[c, 1], csem.at[c, R_H1])
        landed(GA.at[c], csem.at[c, R_CAG])
        pltpu.make_async_copy(GA.at[c], big_hbm.at[core, c], osem.at[2 * c]).wait()
        pltpu.make_async_copy(GB.at[c], big_hbm.at[1 - core, c], osem.at[2 * c + 1]).wait()
    landed(dsm, ssend.at[0])
    landed(dpr, ssend.at[1])
    landed(dpr.at[0:3], ssend.at[2])
    landed(dpr, ssend.at[3])
    pltpu.make_async_copy(dout, small_hbm, osem.at[8]).wait()
    for part in (0, 1):
        rows = slice(part * 512, part * 512 + 512)
        pltpu.make_async_copy(obuf.at[rows], gin_hbm.at[rows], osem.at[9 + part]).wait()


def on_device(features, dw_weight, norm_gain, w_up, w_down, cotangent):
    vm, dma = pltpu.VMEM, pltpu.SemaphoreType.DMA
    any_ = pl.BlockSpec(memory_space=pl.ANY)
    gin, small, big = pl.pallas_call(
        kernel,
        out_shape=(
            jax.ShapeDtypeStruct((PIX, CH), BF16),
            jax.ShapeDtypeStruct((64, CH), F32),
            jax.ShapeDtypeStruct((2, NCH, 4, 16, 16, 256), BF16),
        ),
        in_specs=[any_] * 6,
        out_specs=[any_] * 3,
        scratch_shapes=[
            vm((ROWS, COLS, CH), BF16), vm((PIX, CH), BF16), vm((CH, FF), BF16), vm((FF, CH), BF16),
            vm((49, CH), F32), vm((1, CH), F32),
            vm((4, 14, 144, 128), F32), vm((4, 14, 144, 128), F32), vm((4, 49, 8, 128), F32),
            vm((4, PIX, 128), F32), vm((PIX, 128), F32), vm((PIX, CH), BF16),
            vm((PIX, FC), BF16), vm((PIX, FC), BF16), vm((PIX, CH), F32),
            vm((NCH, 2, 2, 512, 256), F32), vm((ROWS, COLS, CH), BF16), vm((PIX, CH), BF16),
            vm((2, 2, 8, 8, CH), BF16), vm((2, 2, 3, COLS, CH), BF16), vm((2, 2, 8, 8, CH), BF16), vm((2, 4, 3, 8, CH), BF16),
            vm((NCH, 4, 16, 16, 256), BF16), vm((NCH, 4, 16, 16, 256), BF16), vm((NCH, 4, 16, 16, 256), BF16),
            vm((NCH, 2, 8, 16, 256), BF16), vm((NCH, 2, 16, 16, 256), BF16), vm((NCH, 2, 16, 16, 256), BF16),
            vm((NCH, 16, 16, 256), BF16), vm((NCH, 15, 16, 256), BF16),
            vm((NCH, 4, 16, 16, 256), BF16), vm((NCH, 4, 16, 16, 256), BF16),
            vm((4, 64, 128), F32), vm((16, 16, 128), F32), vm((16, 16, 128), F32), vm((16, 16, 128), F32),
            vm((15, 16, 128), F32), vm((4, 16, 128), F32), vm((16, 16, 128), F32), vm((64, CH), F32),
            dma((6,)), dma((2, 8)), dma((2, 8)), dma((NCH, 12)), dma((NCH, 12)), dma((4,)), dma((4,)), dma((11,)),
        ],
        compiler_params=pltpu.CompilerParams(
            collective_id=0, has_side_effects=True, vmem_limit_bytes=66_000_000
        ),
        name="block_backward",
    )(features, dw_weight, norm_gain.reshape(1, CH), w_up, w_down, cotangent.reshape(PIX, CH))
    big = big.reshape(2, NCH, 2, 512, 256)
    grad_down = big[0].transpose(0, 2, 1, 3).reshape(FF, CH).astype(F32)
    grad_up = big[1].transpose(2, 0, 1, 3).reshape(CH, FF).astype(F32)
    return gin.reshape(ROWS, COLS, CH), small[:49], small[49], grad_up, grad_down


def solution(mesh):
    return jax.shard_map(
        on_device,
        mesh=mesh,
        in_specs=(P("rows", "cols", None), P(), P(), P(), P(), P("rows", "cols", None)),
        out_specs=(P("rows", "cols", None), P(), P(), P(), P()),
        check_vma=False,
    )
```

```python
import jax
import jax.numpy as jnp
from jax import lax
from jax.experimental import pallas as pl
from jax.experimental.pallas import tpu as pltpu
from jax.sharding import PartitionSpec as P

EPS = 1e-06
ROWS, COLS, CH, FF = 8, 128, 512, 2048
PIX = ROWS * COLS
CHUNKS = (512, 512, 512, 256, 256)
STARTS = tuple(sum(CHUNKS[:n]) for n in range(len(CHUNKS)))
LEFT = 8
F32, BF16 = jnp.float32, jnp.bfloat16
MESH = pl.DeviceIdType.MESH
FIRST_AXIS = ((0, 2), (1, 0), (2, 1), (0, 2), (2, 0))
SIDES = ((-1, 0), (1, 0), (0, -1), (0, 1), (-1, -1), (-1, 1), (1, -1), (1, 1))
(R_CORE, R_A0, R_A1, R_B0, R_B1, R_PRS, R_PAG, R_G0, R_G1, R_H0, R_H1, R_CAG) = range(12)


def direct(c):
    return c > 1


def kernel(*refs):
    refs = list(refs)

    def take(n):
        out = refs[:n]
        del refs[:n]
        return out

    feat_hbm, dww_hbm, gain_hbm, wup_hbm, wdn_hbm, cot_hbm = take(6)
    gin_hbm, small_hbm = take(2)
    big_hbm = take(len(CHUNKS))
    fbuf, cbuf, wup, wdn, dww, gainb, xf, gp, wb, cv, nv, invb, sc = take(13)
    act, gh, gs, gb, obuf, scol, hrow, hcol, hcor = take(9)
    gd, dsm, dpr, dax, dga, dout = take(6)
    G, csend, crecv, M, axa, axs, axb, pls, plr, GA, GB = zip(*[take(11) for _ in CHUNKS])
    ld, hsend, hrecv, csem, rsem, ssend, srecv, osem = take(8)

    ra, ca = lax.axis_index("rows"), lax.axis_index("cols")
    core = ra % 2
    y, z, x = (ra // 2) % 4, ra // 8, ca

    def device(x_, y_, z_, core_):
        return ((z_ * 4 + y_) * 2 + core_, x_)

    partner = device(x, y, z, 1 - core)

    def side(dr, dc):
        return ((ra + dr + 32) % 32, (ca + dc + 4) % 4)

    def plane_peer(d, axis):
        ix, iy, iz = axis
        u, v = ix * y + iy * z + iz * x, ix * z + iy * x + iz * y
        u2, v2 = (u + d // 4) % 4, (v + d % 4) % 4
        return (
            device(
                ix * x + iy * v2 + iz * u2,
                ix * u2 + iy * y + iz * v2,
                ix * v2 + iy * u2 + iz * z,
                core,
            ),
            u2 * 4 + v2,
        )

    def plane_pos(axis):
        ix, iy, iz = axis
        return (ix * y + iy * z + iz * x) * 4 + ix * z + iy * x + iz * y

    def pair_peer(d):
        x2, y2, core2 = (x + d // 8) % 4, (y + (d // 2) % 4) % 4, (core + d % 2) % 2
        return device(x2, y2, z, core2), (x2 * 4 + y2) * 2 + core2

    def axis_of(c):
        a0, a1 = FIRST_AXIS[c]
        return tuple((a0 == n) * (1 - core) + (a1 == n) * core for n in range(3))

    def along(axis, step):
        ix, iy, iz = axis
        return device(
            (x + step * ix) % 4, (y + step * iy) % 4, (z + step * iz) % 4, core
        )

    def remote(src, dst, send, recv, to):
        return pltpu.make_async_remote_copy(
            src_ref=src, dst_ref=dst, send_sem=send, recv_sem=recv, device_id=to, device_id_type=MESH
        )

    def landed(ref, sem):
        pltpu.make_async_copy(ref, ref, sem).wait()

    loads = [
        pltpu.make_async_copy(s, d, ld.at[n])
        for n, (s, d) in enumerate(
            ((feat_hbm, fbuf), (dww_hbm, dww), (gain_hbm, gainb), (cot_hbm, cbuf), (wup_hbm, wup), (wdn_hbm, wdn))
        )
    ]
    for c_ in loads:
        c_.start()
    barrier = pltpu.get_barrier_semaphore()
    for dr, dc in SIDES:
        pl.semaphore_signal(barrier, inc=1, device_id=side(dr, dc), device_id_type=MESH)

    @pl.loop(1, 32)
    def _(d):
        pl.semaphore_signal(barrier, inc=1, device_id=pair_peer(d)[0], device_id_type=MESH)

    for axis in ((1, 0, 0), (0, 1, 0)):
        @pl.loop(1, 16)
        def _(d, axis=axis):
            pl.semaphore_signal(barrier, inc=1, device_id=plane_peer(d, axis)[0], device_id_type=MESH)

    for c_ in loads[:3]:
        c_.wait()

    def edges(pad, phase):
        for n, start in ((0, LEFT), (1, LEFT + COLS - 8)):
            for cc in range(4):
                scol[phase, n, :, :, cc * 128 : cc * 128 + 128] = pad[
                    cc, 3 : 3 + ROWS, start : start + 8, :
                ].astype(BF16)

    with jax.named_scope("widen"):
        @pl.loop(0, ROWS)
        def _(r):
            for cc in range(4):
                xf[cc, 3 + r, LEFT : LEFT + COLS, :] = fbuf[r, :, cc * 128 : cc * 128 + 128].astype(F32)

        edges(xf, 0)
        for cc in range(4):
            gd[cc, 48:64, :] = jnp.zeros((16, 128), F32)

    with jax.named_scope("entry"):
        pl.semaphore_wait(barrier, len(SIDES) + 31 + 30)

    def halo_copies(phase, rows_src):
        out = []
        for n, (dr, dc) in enumerate(SIDES):
            rs = slice(0, 3) if dr < 0 else slice(5, 8)
            if dc == 0:
                src, dst = rows_src.at[rs], hrow.at[phase, n]
            elif dr == 0:
                src, dst = scol.at[phase, n - 2], hcol.at[phase, n - 2]
            else:
                src, dst = scol.at[phase, 0 if dc < 0 else 1, rs], hcor.at[phase, n - 4]
            if dc == 0 and phase == 1:
                cols = [pl.ds(32 * k, 32) for k in range(4)]
                out.append([
                    remote(src.at[:, k], dst.at[:, k], hsend.at[1, n], hrecv.at[1, n], side(dr, dc)) for k in cols
                ])
            else:
                out.append([remote(src, dst, hsend.at[phase, n], hrecv.at[phase, n], side(dr, dc))])
        return out

    def halo_landed(phase, n):
        buf = hrow.at[phase, n] if n < 2 else hcol.at[phase, n - 2] if n < 4 else hcor.at[phase, n - 4]
        landed(buf, hrecv.at[phase, n])

    valid = {
        -1: jnp.where(ra < 31, 1.0, 0.0).astype(F32),
        1: jnp.where(ra > 0, 1.0, 0.0).astype(F32),
    }
    valid_c = {
        -1: jnp.where(ca < 3, 1.0, 0.0).astype(F32),
        1: jnp.where(ca > 0, 1.0, 0.0).astype(F32),
    }

    def halo_cols(phase, pad):
        for n in (2, 3):
            halo_landed(phase, n)
            dc = SIDES[n][1]
            start = LEFT + COLS if dc < 0 else LEFT - 8
            for cc in range(4):
                pad[cc, 3 : 3 + ROWS, start : start + 8, :] = (
                    hcol[phase, n - 2, :, :, cc * 128 : cc * 128 + 128].astype(F32) * valid_c[dc]
                )

    def halo_rows(phase, pad):
        for n in (0, 1):
            halo_landed(phase, n)
            dr = SIDES[n][0]
            r0 = 3 + ROWS if dr < 0 else 0
            for r in range(3):
                for cc in range(4):
                    pad[cc, r0 + r, LEFT : LEFT + COLS, :] = (
                        hrow[phase, n, r, :, cc * 128 : cc * 128 + 128].astype(F32) * valid[dr]
                    )
        for n in range(4, 8):
            halo_landed(phase, n)
            dr, dc = SIDES[n]
            r0 = 3 + ROWS if dr < 0 else 0
            start = LEFT + COLS if dc < 0 else LEFT - 8
            for cc in range(4):
                pad[cc, r0 : r0 + 3, start : start + 8, :] = hcor[
                    phase, n - 4, :, :, cc * 128 : cc * 128 + 128
                ].astype(F32) * (valid[dr] * valid_c[dc])

    def conv(pad, flip, cc, cb, inner):
        rhos = range(3, 11) if inner else (0, 1, 2, 11, 12, 13)
        rows = range(ROWS) if inner else (0, 1, 2, 5, 6, 7)
        base = cb * 32

        def at(r, b):
            return pl.ds(pl.multiple_of(r * COLS + base + 8 * b, 8), 8)

        def body(j, acc):
            acc = dict(zip([(r, b) for r in rows for b in range(4)], acc))
            w = [wb[cc, (48 - 7 * i - j) if flip else (7 * i + j)] for i in range(7)]
            for rho in rhos:
                for b in range(4):
                    v = pad[cc, rho, pl.ds(base + (8 * b + LEFT - 3) + j, 8), :]
                    for r in rows:
                        if 0 <= rho - r <= 6:
                            acc[r, b] = acc[r, b] + v * w[rho - r]
            return tuple(acc.values())

        if inner:
            start = tuple(jnp.zeros((8, 128), F32) for r in rows for b in range(4))
        else:
            start = tuple(cv[cc, at(r, b), :] for r in rows for b in range(4))
        acc = lax.fori_loop(0, 7, body, start, unroll=1 if inner else 7)
        for n, (r, b) in enumerate([(r, b) for r in rows for b in range(4)]):
            cv[cc, at(r, b), :] = acc[n]

    halo = halo_copies(0, fbuf)
    with jax.named_scope("taps"):
        for n in (2, 3, 0, 1, 4, 5, 6, 7):
            halo[n][0].start()

        for t in range(49):
            for cc in range(4):
                wb[cc, t] = jnp.broadcast_to(dww[t : t + 1, cc * 128 : cc * 128 + 128], (8, 128))

    with jax.named_scope("fconv_mid"):
        @pl.loop(0, 8)
        def _(t):
            conv(xf, False, t // 2, 1 + t % 2, True)

    with jax.named_scope("fhalo_c"):
        halo_cols(0, xf)

    with jax.named_scope("fconv_side"):
        @pl.loop(0, 8)
        def _(t):
            conv(xf, False, t // 2, 3 * (t % 2), True)

    with jax.named_scope("fhalo_r"):
        halo_rows(0, xf)

    with jax.named_scope("fconv_out"):
        @pl.loop(0, 16)
        def _(t):
            conv(xf, False, t // 4, t % 4, False)

    with jax.named_scope("norm"):
        def norm(t, carry):
            ps = pl.ds(pl.multiple_of(t * 64, 64), 64)
            v = [cv[cc, ps, :] for cc in range(4)]
            mean = jnp.sum(v[0] + v[1] + v[2] + v[3], axis=1, keepdims=True) * (1.0 / CH)
            v = [a - mean for a in v]
            sq = [a * a for a in v]
            inv = lax.rsqrt(jnp.sum(sq[0] + sq[1] + sq[2] + sq[3], axis=1, keepdims=True) * (1.0 / CH) + EPS)
            invb[ps, :] = jnp.broadcast_to(inv, (64, 128))
            for cc in range(4):
                n_ = v[cc] * inv
                nv[cc, ps, :] = n_
                sc[ps, cc * 128 : cc * 128 + 128] = (n_ * gainb[:, cc * 128 : cc * 128 + 128]).astype(BF16)
            return carry

        lax.fori_loop(0, 16, norm, 0, unroll=2)

    for c_ in loads[3:]:
        c_.wait()

    def mlp_a(c, half):
        w = CHUNKS[c]
        fs = slice(STARTS[c], STARTS[c] + w)
        for pb in (2 * half, 2 * half + 1):
            ps = slice(pb * 256, pb * 256 + 256)
            h = jnp.dot(sc[ps, :], wup[:, fs], preferred_element_type=F32)
            ga = lax.dot_general(cbuf[ps, :], wdn[fs, :], (((1,), (1,)), ((), ())), preferred_element_type=F32)
            phi = 0.5 * (1.0 + lax.erf(h * 0.7071067811865476))
            act[ps, 0:w] = (h * phi).astype(BF16)
            e = jnp.exp(-0.5 * h * h) * 0.3989422804014327
            gh[ps, fs] = (ga * (phi + h * e)).astype(BF16)

    def put(c, slot, value):
        w, rows = CHUNKS[c] // 2, value.shape[0]
        for n in range(1024 // rows):
            G[c][slot, n * rows : (n + 1) * rows, :] = value[:, n * w : (n + 1) * w]

    def mlp_down(c):
        put(c, core, lax.dot_general(
            act[:, 0 : CHUNKS[c]], cbuf[...], (((0,), (0,)), ((), ())), preferred_element_type=F32))

    def mlp_up(c):
        fs = slice(STARTS[c], STARTS[c] + CHUNKS[c])
        put(c, 1 - core, lax.dot_general(
            sc[...], gh[:, fs], (((0,), (0,)), ((), ())), preferred_element_type=F32))

    def mlp_back(q):
        ps = slice(q * 256, q * 256 + 256)
        gs[ps, :] = lax.dot_general(gh[ps, :], wup[...], (((1,), (1,)), ((), ())), preferred_element_type=F32)

    def blocks(fn):
        @pl.loop(0, 8)
        def _(t):
            fn(t // 2, pl.ds((t % 2) * 8, 8), pl.ds(pl.multiple_of(t * 128, 128), 128))

    def place(c):
        axis = axis_of(c)
        return axis, axis[0] * x + axis[1] * y + axis[2] * z

    def send(c, n, src, dst, to):
        remote(src, dst, csem.at[c, n], rsem.at[c, n], to).start()

    def arrived(c, n, ref):
        landed(ref, rsem.at[c, n])

    def ch_core(c):
        def go(a, n, rows):
            csend[c][a, n] = G[c][1, rows, :].reshape(8, 16, CHUNKS[c] // 2).astype(BF16)
        blocks(go)
        send(c, R_CORE, csend[c], crecv[c], partner)

    def ch_axis(c):
        arrived(c, R_CORE, crecv[c])
        axis, p = place(c)
        def go(a, n, rows):
            M[c][a, n] = (
                G[c][0, rows, :].reshape(8, 16, CHUNKS[c] // 2) + crecv[c][a, n].astype(F32)
            ).astype(BF16)
        blocks(go)
        if direct(c):
            for d in (2, 1, 3):
                send(c, R_A0, M[c].at[(p + d) % 4], axb[c].at[d - 1], along(axis, d))
        else:
            far = (p + 2) % 4
            send(c, R_A0, M[c].at[far, 0:8], axa[c].at[0], along(axis, 1))
            send(c, R_A1, M[c].at[far, 8:16], axa[c].at[1], along(axis, 3))

    def ch_axis2(c):
        axis, p = place(c)
        arrived(c, R_A0, axa[c].at[0])
        arrived(c, R_A1, axa[c].at[1])
        right, left = (p + 1) % 4, (p + 3) % 4
        axs[c][0, 0:8] = (M[c][right, 0:8].astype(F32) + axa[c][0].astype(F32)).astype(BF16)
        axs[c][0, 8:16] = M[c][right, 8:16]
        send(c, R_B0, axs[c].at[0], axb[c].at[0], along(axis, 1))
        axs[c][1, 0:8] = M[c][left, 0:8]
        axs[c][1, 8:16] = (M[c][left, 8:16].astype(F32) + axa[c][1].astype(F32)).astype(BF16)
        send(c, R_B1, axs[c].at[1], axb[c].at[1], along(axis, 3))

    def ch_plane(c):
        axis, p = place(c)
        if direct(c):
            arrived(c, R_A0, axb[c])
        else:
            arrived(c, R_B0, axb[c].at[0])
            arrived(c, R_B1, axb[c].at[1])
        total = M[c][p].astype(F32)
        for n in range(3 if direct(c) else 2):
            total = total + axb[c][n].astype(F32)
        pls[c][...] = total.astype(BF16)

        @pl.loop(1, 16, unroll=5)
        def _(d):
            to, pos = plane_peer(d, axis)
            send(c, R_PRS, pls[c].at[pos], plr[c].at[d - 1], to)

    def ch_share(c):
        axis, p = place(c)
        pos = plane_pos(axis)
        arrived(c, R_PRS, plr[c])
        total = pls[c][pos].astype(F32)
        for d in range(15):
            total = total + plr[c][d].astype(F32)
        GA[c][p, pos] = total.astype(BF16)

        @pl.loop(1, 16, unroll=5)
        def _(d):
            to, _ = plane_peer(d, axis)
            send(c, R_PAG, GA[c].at[p, pos], GA[c].at[p, pos], to)

    def ch_back(c):
        axis, p = place(c)
        arrived(c, R_PAG, plr[c])
        if direct(c):
            for d in (2, 1, 3):
                send(c, R_G0, GA[c].at[p], GA[c].at[p], along(axis, d))
        else:
            send(c, R_G0, GA[c].at[p], GA[c].at[p], along(axis, 1))
            send(c, R_G1, GA[c].at[p], GA[c].at[p], along(axis, 3))
        send(c, R_CAG, GA[c].at[p], GB[c].at[p], partner)

    def ch_back2(c):
        axis, p = place(c)
        right, left = (p + 1) % 4, (p + 3) % 4
        arrived(c, R_G0, GA[c].at[left])
        arrived(c, R_G1, GA[c].at[right])
        a, b = GA[c].at[left, 0:8], GA[c].at[right, 8:16]
        send(c, R_H0, a, a, along(axis, 1))
        send(c, R_H1, b, b, along(axis, 3))
        for q in (left, right):
            send(c, R_CAG, GA[c].at[q], GB[c].at[q], partner)

    def ch_pair(c):
        axis, p = place(c)
        if direct(c):
            arrived(c, R_G0, axb[c])
            for d in (1, 2, 3):
                q = (p + d) % 4
                send(c, R_CAG, GA[c].at[q], GB[c].at[q], partner)
        else:
            arrived(c, R_H0, axa[c].at[0])
            arrived(c, R_H1, axa[c].at[1])
            far = (p + 2) % 4
            send(c, R_CAG, GA[c].at[far], GB[c].at[far], partner)
        pltpu.make_async_copy(GA[c], big_hbm[c].at[core], osem.at[2 * c]).start()

    def ch_end(c):
        arrived(c, R_CAG, GB[c])
        pltpu.make_async_copy(GB[c], big_hbm[c].at[1 - core], osem.at[2 * c + 1]).start()

    def ln_back(quarter):
        def body(t, part):
            ps = slice(quarter * 256 + t * 64, quarter * 256 + t * 64 + 64)
            inv = invb[ps, :]
            ns = [nv[cc, ps, :] for cc in range(4)]
            gv = [gs[ps, cc * 128 : cc * 128 + 128] for cc in range(4)]
            prod = [g * n for g, n in zip(gv, ns)]
            part = tuple(
                q + jnp.sum(pr.reshape(8, 8, 128), axis=0) for q, pr in zip(part, prod)
            )
            gains = [gainb[:, cc * 128 : cc * 128 + 128] for cc in range(4)]
            gn = [g * k for g, k in zip(gv, gains)]
            gm = [pr * k for pr, k in zip(prod, gains)]
            m1 = jnp.sum(gn[0] + gn[1] + gn[2] + gn[3], axis=1, keepdims=True) * (1.0 / CH)
            m2 = jnp.sum(gm[0] + gm[1] + gm[2] + gm[3], axis=1, keepdims=True) * (1.0 / CH)
            r, c0 = 2 * quarter + t // 2, (t % 2) * 64
            for cc in range(4):
                g = (inv * (gn[cc] - m1 - ns[cc] * m2)).astype(BF16)
                gb[r, c0 : c0 + 64, cc * 128 : cc * 128 + 128] = g
                gp[cc, 3 + r, LEFT + c0 : LEFT + c0 + 64, :] = g.astype(F32)
            return part

        part = tuple(jnp.zeros((8, 128), F32) for _ in range(4))
        for t in range(4):
            part = body(t, part)
        for cc in range(4):
            row = jnp.sum(part[cc], axis=0, keepdims=True)
            gd[cc, 49:50, :] = row if quarter == 0 else gd[cc, 49:50, :] + row

    back = halo_copies(1, gb)

    def send_back():
        edges(gp, 1)
        for n in (2, 3, 4, 5, 6, 7):
            back[n][0].start()

    def send_rows(k):
        back[0][k].start()
        back[1][k].start()

    def gdw(cc, js):
        @pl.loop(js[0], js[1])
        def _(j):
            def body(cb, acc):
                acc = list(acc)
                base = cb * 64
                for b in range(8):
                    gv = [gp[cc, 3 + r, pl.ds(pl.multiple_of(base + LEFT + 8 * b, 8), 8), :] for r in range(8)]
                    for rho in range(14):
                        v = xf[cc, rho, pl.ds(base + (8 * b + LEFT - 3) + j, 8), :]
                        for r in range(max(0, rho - 6), min(8, rho + 1)):
                            acc[rho - r] = acc[rho - r] + v * gv[r]
                return tuple(acc)

            acc = lax.fori_loop(0, 2, body, tuple(jnp.zeros((8, 128), F32) for _ in range(7)))
            for i in range(7):
                gd[cc, pl.ds(7 * i + j, 1), :] = jnp.sum(acc[i], axis=0, keepdims=True)

    zaxis = (0, 0, 1)
    mine = (x * 4 + y) * 2 + core
    OUT = 2 * len(CHUNKS)

    def sm_scatter():
        for cc in range(4):
            for tb in range(8):
                dsm[8 * cc + tb] = gd[cc, 8 * tb : 8 * tb + 8, :]

        @pl.loop(1, 32)
        def _(d):
            to, pos = pair_peer(d)
            remote(dsm.at[pos], dpr.at[d - 1], ssend.at[0], srecv.at[0], to).start()

    def sm_axis():
        landed(dpr, srecv.at[0])
        total = dsm[mine]
        for d in range(31):
            total = total + dpr[d]
        dax[z] = total
        for step in (2, 1, 3):
            remote(dax.at[z], dax.at[z], ssend.at[1], srecv.at[1], along(zaxis, step)).start()

    def sm_share():
        landed(dpr.at[0:3], srecv.at[1])
        dga[mine] = dax[0] + dax[1] + dax[2] + dax[3]

        @pl.loop(1, 32)
        def _(d):
            to, _ = pair_peer(d)
            remote(dga.at[mine], dga.at[mine], ssend.at[2], srecv.at[2], to).start()

    def sm_end():
        landed(dpr, srecv.at[2])
        for cc in range(4):
            for tb in range(8):
                dout[8 * tb : 8 * tb + 8, cc * 128 : cc * 128 + 128] = dga[8 * cc + tb]
        pltpu.make_async_copy(dout, small_hbm, osem.at[OUT]).start()

    def gin_inner(cb, half):
        @pl.loop(2 * half, 2 * half + 2)
        def _(t):
            conv(gp, True, t, cb, True)

    def gin_outer(cb):
        @pl.loop(0, 4)
        def _(t):
            conv(gp, True, t, cb, False)

    def gin_store(part):
        @pl.loop(part * 8, part * 8 + 8)
        def _(t):
            ps = pl.ds(pl.multiple_of(t * 64, 64), 64)
            for cc in range(4):
                cs = slice(cc * 128, cc * 128 + 128)
                obuf[ps, cs] = (cbuf[ps, cs].astype(F32) + cv[cc, ps, :]).astype(BF16)
        rows = slice(part * 512, part * 512 + 512)
        pltpu.make_async_copy(obuf.at[rows], gin_hbm.at[rows], osem.at[OUT + 1 + part]).start()

    work = []
    chains = {}
    for c, w in enumerate(CHUNKS):
        k = w / 512
        work += [(0.75 * k, "mlp_a", lambda c=c: mlp_a(c, 0), None), (0.75 * k, "mlp_a", lambda c=c: mlp_a(c, 1), None)]
        work += [(0.73 * k, "mlp_down", lambda c=c: mlp_down(c), None), (0.73 * k, "mlp_up", lambda c=c: mlp_up(c), c)]
        if direct(c):
            steps = (
                (0.0, ch_core), (2.2, ch_axis), (5.5, ch_plane), (7.0, ch_share), (6.0, ch_back), (6.0, ch_pair), (2.5, ch_end)
            )
        else:
            steps = (
                (0.0, ch_core), (2.5, ch_axis), (4.0, ch_axis2), (5.0, ch_plane), (7.0, ch_share),
                (6.0, ch_back), (5.0, ch_back2), (5.0, ch_pair), (2.5, ch_end),
            )
        chains[c] = [(gap, fn.__name__, lambda fn=fn, c=c: fn(c)) for gap, fn in steps]
    def both(q):
        if q < 4:
            mlp_back(q)
        if q > 0:
            ln_back(q - 1)

    work += [(0.73, "back", lambda q=q: both(q), None) for q in range(5)]
    work += [(0.1, "send_back", send_back, None)]
    small = len(CHUNKS)
    for cc in range(4):
        work += [(0.8, "gdw", lambda cc=cc: gdw(cc, (0, 3)), None)]
        work += [(0.02, "send_rows", lambda cc=cc: send_rows(cc), None)]
        work += [(0.55, "gdw", lambda cc=cc: gdw(cc, (3, 5)), None)]
        work += [(0.55, "gdw", lambda cc=cc: gdw(cc, (5, 7)), small if cc == 3 else None)]
    steps = ((0.0, sm_scatter), (4.6, sm_axis), (3.6, sm_share), (6.0, sm_end))
    chains[small] = [(gap, fn.__name__, fn) for gap, fn in steps]
    for n, cb in enumerate((1, 2, 0, 3)):
        if n == 2:
            work += [(0.05, "halo_c", lambda: halo_cols(1, gp), None)]
        work += [(0.85, "gin_in", lambda cb=cb, half=half: gin_inner(cb, half), None) for half in (0, 1)]
    work += [(0.15, "halo_r", lambda: halo_rows(1, gp), None)]
    work += [(0.7, "gin_out", lambda cb=cb: gin_outer(cb), None) for cb in range(4)]
    work += [(0.2, "gin_st", lambda: gin_store(0), None), (0.2, "gin_st", lambda: gin_store(1), None)]

    now = 0.0
    due = []

    def serve(limit):
        nonlocal now
        while due and (limit is None or min(due)[0] <= limit):
            when, key, n = min(due)
            due.remove((when, key, n))
            now = max(now, when) + 0.1
            with jax.named_scope(f"{chains[key][n][1]}_{key}"):
                chains[key][n][2]()
            if n + 1 < len(chains[key]):
                due.append((now + chains[key][n + 1][0], key, n + 1))

    for cost, name, fn, opens in work:
        with jax.named_scope(name):
            fn()
        now += cost
        if opens is not None:
            due.append((now, opens, 0))
        serve(now)
    serve(None)

    with jax.named_scope("drain"):
        for phase in (0, 1):
            for n in range(8):
                buf = hrow.at[phase, n] if n < 2 else hcol.at[phase, n - 2] if n < 4 else hcor.at[phase, n - 4]
                landed(buf, hsend.at[phase, n])
        for c in range(len(CHUNKS)):
            sent = [(R_CORE, csend[c]), (R_PRS, plr[c]), (R_PAG, plr[c]), (R_CAG, GA[c])]
            if direct(c):
                sent += [(R_A0, axb[c]), (R_G0, axb[c])]
            else:
                sent += [(R_A0, axa[c].at[0]), (R_A1, axa[c].at[1]), (R_B0, axb[c].at[0]), (R_B1, axb[c].at[1])]
                sent += [(R_G0, axb[c].at[0]), (R_G1, axb[c].at[1]), (R_H0, axa[c].at[0]), (R_H1, axa[c].at[1])]
            for n, ref in sent:
                landed(ref, csem.at[c, n])
            pltpu.make_async_copy(GA[c], big_hbm[c].at[core], osem.at[2 * c]).wait()
            pltpu.make_async_copy(GB[c], big_hbm[c].at[1 - core], osem.at[2 * c + 1]).wait()
        landed(dpr, ssend.at[0])
        landed(dpr.at[0:3], ssend.at[1])
        landed(dpr, ssend.at[2])
        pltpu.make_async_copy(dout, small_hbm, osem.at[OUT]).wait()
        for part in (0, 1):
            rows = slice(part * 512, part * 512 + 512)
            pltpu.make_async_copy(obuf.at[rows], gin_hbm.at[rows], osem.at[OUT + 1 + part]).wait()


def finish_kernel(*refs):
    refs = list(refs)
    n_ch = len(CHUNKS)
    gin_hbm, small_hbm = refs[:2]
    big_hbm = refs[2 : 2 + n_ch]
    gout_hbm, dw_hbm, gain_hbm, up_hbm, down_hbm, gbuf, sbuf, dbuf, kbuf = refs[2 + n_ch : 11 + n_ch]
    narrow = refs[11 + n_ch : 11 + 2 * n_ch]
    downs = refs[11 + 2 * n_ch : 11 + 3 * n_ch]
    ups = refs[11 + 3 * n_ch : 11 + 4 * n_ch]
    isem, osem = refs[11 + 4 * n_ch :]
    ins = [
        [pltpu.make_async_copy(big_hbm[c].at[s], narrow[c].at[s], isem.at[2 * c + s]) for s in range(2)]
        for c in range(n_ch)
    ]
    for pair in ins:
        for c_ in pair:
            c_.start()
    first = pltpu.make_async_copy(gin_hbm, gbuf, isem.at[2 * n_ch])
    second = pltpu.make_async_copy(small_hbm, sbuf, isem.at[2 * n_ch + 1])
    first.start()
    second.start()
    outs = []

    def put(src, dst):
        outs.append(pltpu.make_async_copy(src, dst, osem.at[len(outs)]))
        outs[-1].start()

    for c, w in enumerate(CHUNKS):
        half = w // 2
        for s in range(2):
            ins[c][s].wait()
            wide = (downs, ups)[s][c]
            rows = wide.shape[0]
            step = min(rows, 1024) // 4

            @pl.loop(0, 4)
            def _(t):
                rs = pl.ds(pl.multiple_of(t * step, step), step)
                for n in range(1024 // rows):
                    wide[rs, n * half : (n + 1) * half] = narrow[c][
                        s, pl.ds(pl.multiple_of(n * rows + t * step, step), step), :
                    ].astype(F32)

            part = pl.ds(STARTS[c], w)
            put(wide, down_hbm.at[part] if s == 0 else up_hbm.at[:, part])
    first.wait()
    put(gbuf, gout_hbm)
    second.wait()
    dbuf[...] = sbuf[0:49, :]
    kbuf[...] = sbuf[49:50, :]
    put(dbuf, dw_hbm)
    put(kbuf, gain_hbm)
    for c_ in outs:
        c_.wait()


def finish(gin, small, big):
    vm, dma = pltpu.VMEM, pltpu.SemaphoreType.DMA
    any_ = pl.BlockSpec(memory_space=pl.ANY)
    n_ch = len(CHUNKS)
    gin, dw, gain, up, down = pl.pallas_call(
        finish_kernel,
        out_shape=(
            jax.ShapeDtypeStruct((PIX, CH), BF16),
            jax.ShapeDtypeStruct((49, CH), F32),
            jax.ShapeDtypeStruct((1, CH), F32),
            jax.ShapeDtypeStruct((CH, FF), F32),
            jax.ShapeDtypeStruct((FF, CH), F32),
        ),
        in_specs=[any_] * (2 + n_ch),
        out_specs=[any_] * 5,
        scratch_shapes=[vm((PIX, CH), BF16), vm((64, CH), F32), vm((49, CH), F32), vm((1, CH), F32)]
        + [vm((2, 1024, w // 2), BF16) for w in CHUNKS]
        + [vm((w, CH), F32) for w in CHUNKS]
        + [vm((CH, w), F32) for w in CHUNKS]
        + [dma((2 * n_ch + 2,)), dma((2 * n_ch + 3,))],
        compiler_params=pltpu.CompilerParams(vmem_limit_bytes=66_000_000),
        name="finish",
    )(gin, small, *[b.reshape(2, 1024, w // 2) for b, w in zip(big, CHUNKS)])
    return gin.reshape(ROWS, COLS, CH), dw, gain.reshape(CH), up, down


def on_device(features, dw_weight, norm_gain, w_up, w_down, cotangent):
    vm, dma = pltpu.VMEM, pltpu.SemaphoreType.DMA
    any_ = pl.BlockSpec(memory_space=pl.ANY)
    n_ch = len(CHUNKS)
    comm = []
    for c, w in enumerate(CHUNKS):
        h = w // 2
        whole = vm((4, 16, 16, h), BF16)
        comm += [vm((2, 1024, h), F32), whole, whole, whole]
        comm += [vm((2, 8, 16, h), BF16), vm((2, 16, 16, h), BF16), vm((3 if direct(c) else 2, 16, 16, h), BF16)]
        comm += [vm((16, 16, h), BF16), vm((15, 16, h), BF16), whole, whole]
    gin, small, *big = pl.pallas_call(
        kernel,
        out_shape=(
            jax.ShapeDtypeStruct((PIX, CH), BF16),
            jax.ShapeDtypeStruct((64, CH), F32),
            *[jax.ShapeDtypeStruct((2, 4, 16, 16, w // 2), BF16) for w in CHUNKS],
        ),
        in_specs=[any_] * 6,
        out_specs=[any_] * (2 + n_ch),
        scratch_shapes=[
            vm((ROWS, COLS, CH), BF16), vm((PIX, CH), BF16), vm((CH, FF), BF16), vm((FF, CH), BF16),
            vm((49, CH), F32), vm((1, CH), F32),
            vm((4, 14, 144, 128), F32), vm((4, 14, 144, 128), F32), vm((4, 49, 8, 128), F32),
            vm((4, PIX, 128), F32), vm((4, PIX, 128), F32), vm((PIX, 128), F32), vm((PIX, CH), BF16),
            vm((PIX, max(CHUNKS)), BF16), vm((PIX, FF), BF16), vm((PIX, CH), F32),
            vm((ROWS, COLS, CH), BF16), vm((PIX, CH), BF16),
            vm((2, 2, 8, 8, CH), BF16), vm((2, 2, 3, COLS, CH), BF16), vm((2, 2, 8, 8, CH), BF16), vm((2, 4, 3, 8, CH), BF16),
            vm((4, 64, 128), F32), vm((32, 8, 128), F32), vm((31, 8, 128), F32), vm((4, 8, 128), F32),
            vm((32, 8, 128), F32), vm((64, CH), F32),
        ]
        + comm
        + [
            dma((6,)), dma((2, 8)), dma((2, 8)), dma((n_ch, 12)), dma((n_ch, 12)), dma((3,)), dma((3,)), dma((2 * n_ch + 3,)),
        ],
        compiler_params=pltpu.CompilerParams(
            collective_id=0, has_side_effects=True, vmem_limit_bytes=67_000_000
        ),
        name="block_backward",
    )(features, dw_weight, norm_gain.reshape(1, CH), w_up, w_down, cotangent.reshape(PIX, CH))
    return finish(gin, small, big)


def solution(mesh):
    return jax.shard_map(
        on_device,
        mesh=mesh,
        in_specs=(P("rows", "cols", None), P(), P(), P(), P(), P("rows", "cols", None)),
        out_specs=(P("rows", "cols", None), P(), P(), P(), P()),
        check_vma=False,
    )
```

```python
import jax
import jax.numpy as jnp
from jax import lax
from jax.experimental import pallas as pl
from jax.experimental.pallas import tpu as pltpu
from jax.sharding import PartitionSpec as P

EPS = 1e-06
ROWS, COLS, CH, FF = 8, 128, 512, 2048
PIX = ROWS * COLS
CHUNKS = (512, 512, 512, 256, 256)
STARTS = tuple(sum(CHUNKS[:n]) for n in range(len(CHUNKS)))
LEFT = 8
F32, BF16 = jnp.float32, jnp.bfloat16
MESH = pl.DeviceIdType.MESH
FIRST_AXIS = ((0, 2), (1, 0), (2, 1), (0, 2), (2, 0))
SIDES = ((-1, 0), (1, 0), (0, -1), (0, 1), (-1, -1), (-1, 1), (1, -1), (1, 1))
(R_CORE, R_A0, R_A1, R_B0, R_B1, R_PRS, R_PAG, R_G0, R_G1, R_H0, R_H1, R_CAG) = range(12)


def direct(c):
    return c > 1


def kernel(*refs):
    refs = list(refs)

    def take(n):
        out = refs[:n]
        del refs[:n]
        return out

    feat_hbm, dww_hbm, gain_hbm, wup_hbm, wdn_hbm, cot_hbm = take(6)
    obuf, dout = take(2)
    GA, GB = take(len(CHUNKS)), take(len(CHUNKS))
    fbuf, cbuf, wup, wdn, dww, gainb, xf, gp, wb, cv, nv, invb, sc = take(13)
    act, gh, gs, gb, scol, hrow, hcol, hcor = take(8)
    gd, dsm, dpr, dax, dga = take(5)
    G, csend, crecv, M, axa, axs, axb, pls, plr = zip(*[take(9) for _ in CHUNKS])
    ld, hsend, hrecv, csem, rsem, ssend, srecv, near = take(8)

    ra, ca = lax.axis_index("rows"), lax.axis_index("cols")
    core = ra % 2
    y, z, x = (ra // 2) % 4, ra // 8, ca

    def device(x_, y_, z_, core_):
        return ((z_ * 4 + y_) * 2 + core_, x_)

    partner = device(x, y, z, 1 - core)

    def side(dr, dc):
        return ((ra + dr + 32) % 32, (ca + dc + 4) % 4)

    def plane_peer(d, axis):
        ix, iy, iz = axis
        u, v = ix * y + iy * z + iz * x, ix * z + iy * x + iz * y
        u2, v2 = (u + d // 4) % 4, (v + d % 4) % 4
        return (
            device(
                ix * x + iy * v2 + iz * u2,
                ix * u2 + iy * y + iz * v2,
                ix * v2 + iy * u2 + iz * z,
                core,
            ),
            u2 * 4 + v2,
        )

    def plane_pos(axis):
        ix, iy, iz = axis
        return (ix * y + iy * z + iz * x) * 4 + ix * z + iy * x + iz * y

    def pair_peer(d):
        x2, y2, core2 = (x + d // 8) % 4, (y + (d // 2) % 4) % 4, (core + d % 2) % 2
        return device(x2, y2, z, core2), (x2 * 4 + y2) * 2 + core2

    def axis_of(c):
        a0, a1 = FIRST_AXIS[c]
        return tuple((a0 == n) * (1 - core) + (a1 == n) * core for n in range(3))

    def along(axis, step):
        ix, iy, iz = axis
        return device(
            (x + step * ix) % 4, (y + step * iy) % 4, (z + step * iz) % 4, core
        )

    def remote(src, dst, send, recv, to):
        return pltpu.make_async_remote_copy(
            src_ref=src, dst_ref=dst, send_sem=send, recv_sem=recv, device_id=to, device_id_type=MESH
        )

    def landed(ref, sem):
        pltpu.make_async_copy(ref, ref, sem).wait()

    loads = [
        pltpu.make_async_copy(s, d, ld.at[n])
        for n, (s, d) in enumerate(
            ((feat_hbm, fbuf), (dww_hbm, dww), (gain_hbm, gainb), (cot_hbm, cbuf), (wup_hbm, wup), (wdn_hbm, wdn))
        )
    ]
    for c_ in loads:
        c_.start()
    barrier = pltpu.get_barrier_semaphore()
    for dr, dc in SIDES:
        pl.semaphore_signal(barrier, inc=1, device_id=side(dr, dc), device_id_type=MESH)

    NEAR = [along(tuple(int(n == k) for n in range(3)), step) for k in range(3) for step in (1, 3)]
    for to in NEAR:
        pl.semaphore_signal(barrier, inc=1, device_id=to, device_id_type=MESH)

    def round_signal(n):
        for to in [partner] + NEAR:
            pl.semaphore_signal(near.at[n], inc=1, device_id=to, device_id_type=MESH)

    def round_wait(n):
        pl.semaphore_wait(near.at[n], 1 + len(NEAR))

    for c_ in loads[:3]:
        c_.wait()

    def edges(pad, phase):
        for n, start in ((0, LEFT), (1, LEFT + COLS - 8)):
            for cc in range(4):
                scol[phase, n, :, :, cc * 128 : cc * 128 + 128] = pad[
                    cc, 3 : 3 + ROWS, start : start + 8, :
                ].astype(BF16)

    with jax.named_scope("widen"):
        @pl.loop(0, ROWS)
        def _(r):
            for cc in range(4):
                xf[cc, 3 + r, LEFT : LEFT + COLS, :] = fbuf[r, :, cc * 128 : cc * 128 + 128].astype(F32)

        edges(xf, 0)
        for cc in range(4):
            gd[cc, 48:64, :] = jnp.zeros((16, 128), F32)

    with jax.named_scope("entry"):
        pl.semaphore_wait(barrier, len(SIDES) + len(NEAR))
        round_signal(0)

    def halo_copies(phase, rows_src):
        out = []
        for n, (dr, dc) in enumerate(SIDES):
            rs = slice(0, 3) if dr < 0 else slice(5, 8)
            if dc == 0:
                src, dst = rows_src.at[rs], hrow.at[phase, n]
            elif dr == 0:
                src, dst = scol.at[phase, n - 2], hcol.at[phase, n - 2]
            else:
                src, dst = scol.at[phase, 0 if dc < 0 else 1, rs], hcor.at[phase, n - 4]
            if dc == 0 and phase == 1:
                cols = [pl.ds(32 * k, 32) for k in range(4)]
                out.append([
                    remote(src.at[:, k], dst.at[:, k], hsend.at[1, n], hrecv.at[1, n], side(dr, dc)) for k in cols
                ])
            else:
                out.append([remote(src, dst, hsend.at[phase, n], hrecv.at[phase, n], side(dr, dc))])
        return out

    def halo_landed(phase, n):
        buf = hrow.at[phase, n] if n < 2 else hcol.at[phase, n - 2] if n < 4 else hcor.at[phase, n - 4]
        landed(buf, hrecv.at[phase, n])

    valid = {
        -1: jnp.where(ra < 31, 1.0, 0.0).astype(F32),
        1: jnp.where(ra > 0, 1.0, 0.0).astype(F32),
    }
    valid_c = {
        -1: jnp.where(ca < 3, 1.0, 0.0).astype(F32),
        1: jnp.where(ca > 0, 1.0, 0.0).astype(F32),
    }

    def halo_cols(phase, pad):
        for n in (2, 3):
            halo_landed(phase, n)
            dc = SIDES[n][1]
            start = LEFT + COLS if dc < 0 else LEFT - 8
            for cc in range(4):
                pad[cc, 3 : 3 + ROWS, start : start + 8, :] = (
                    hcol[phase, n - 2, :, :, cc * 128 : cc * 128 + 128].astype(F32) * valid_c[dc]
                )

    def halo_rows(phase, pad):
        for n in (0, 1):
            halo_landed(phase, n)
            dr = SIDES[n][0]
            r0 = 3 + ROWS if dr < 0 else 0
            for r in range(3):
                for cc in range(4):
                    pad[cc, r0 + r, LEFT : LEFT + COLS, :] = (
                        hrow[phase, n, r, :, cc * 128 : cc * 128 + 128].astype(F32) * valid[dr]
                    )
        for n in range(4, 8):
            halo_landed(phase, n)
            dr, dc = SIDES[n]
            r0 = 3 + ROWS if dr < 0 else 0
            start = LEFT + COLS if dc < 0 else LEFT - 8
            for cc in range(4):
                pad[cc, r0 : r0 + 3, start : start + 8, :] = hcor[
                    phase, n - 4, :, :, cc * 128 : cc * 128 + 128
                ].astype(F32) * (valid[dr] * valid_c[dc])

    def conv(pad, flip, cc, cb, inner):
        rhos = range(3, 11) if inner else (0, 1, 2, 11, 12, 13)
        rows = range(ROWS) if inner else (0, 1, 2, 5, 6, 7)
        base = cb * 32

        def at(r, b):
            return pl.ds(pl.multiple_of(r * COLS + base + 8 * b, 8), 8)

        def body(j, acc):
            acc = dict(zip([(r, b) for r in rows for b in range(4)], acc))
            w = [wb[cc, (48 - 7 * i - j) if flip else (7 * i + j)] for i in range(7)]
            for rho in rhos:
                for b in range(4):
                    v = pad[cc, rho, pl.ds(base + (8 * b + LEFT - 3) + j, 8), :]
                    for r in rows:
                        if 0 <= rho - r <= 6:
                            acc[r, b] = acc[r, b] + v * w[rho - r]
            return tuple(acc.values())

        if inner:
            start = tuple(jnp.zeros((8, 128), F32) for r in rows for b in range(4))
        else:
            start = tuple(cv[cc, at(r, b), :] for r in rows for b in range(4))
        acc = lax.fori_loop(0, 7, body, start, unroll=7)
        for n, (r, b) in enumerate([(r, b) for r in rows for b in range(4)]):
            cv[cc, at(r, b), :] = acc[n]

    halo = halo_copies(0, fbuf)
    with jax.named_scope("taps"):
        for n in (2, 3, 0, 1, 4, 5, 6, 7):
            halo[n][0].start()

        for t in range(49):
            for cc in range(4):
                wb[cc, t] = jnp.broadcast_to(dww[t : t + 1, cc * 128 : cc * 128 + 128], (8, 128))

    with jax.named_scope("fconv_mid"):
        @pl.loop(0, 8)
        def _(t):
            conv(xf, False, t // 2, 1 + t % 2, True)

    with jax.named_scope("fhalo_c"):
        round_wait(0)
        round_signal(1)
        halo_cols(0, xf)

    with jax.named_scope("fconv_side"):
        @pl.loop(0, 8)
        def _(t):
            conv(xf, False, t // 2, 3 * (t % 2), True)

    with jax.named_scope("fhalo_r"):
        round_wait(1)
        round_signal(2)
        halo_rows(0, xf)

    with jax.named_scope("fconv_out"):
        @pl.loop(0, 16)
        def _(t):
            conv(xf, False, t // 4, t % 4, False)

    round_wait(2)
    round_signal(3)

    def norm(quarter):
        for t in range(4):
            ps = slice(quarter * 256 + t * 64, quarter * 256 + t * 64 + 64)
            v = [cv[cc, ps, :] for cc in range(4)]
            mean = jnp.sum(v[0] + v[1] + v[2] + v[3], axis=1, keepdims=True) * (1.0 / CH)
            v = [a - mean for a in v]
            sq = [a * a for a in v]
            inv = lax.rsqrt(jnp.sum(sq[0] + sq[1] + sq[2] + sq[3], axis=1, keepdims=True) * (1.0 / CH) + EPS)
            invb[ps, :] = jnp.broadcast_to(inv, (64, 128))
            for cc in range(4):
                n_ = v[cc] * inv
                nv[cc, ps, :] = n_
                sc[ps, cc * 128 : cc * 128 + 128] = (n_ * gainb[:, cc * 128 : cc * 128 + 128]).astype(BF16)

    for c_ in loads[3:]:
        c_.wait()

    def last_round():
        round_wait(3)

    def mlp_a(c, pbs):
        w = CHUNKS[c]
        fs = slice(STARTS[c], STARTS[c] + w)
        for pb in pbs:
            ps = slice(pb * 256, pb * 256 + 256)
            h = jnp.dot(sc[ps, :], wup[:, fs], preferred_element_type=F32)
            ga = lax.dot_general(cbuf[ps, :], wdn[fs, :], (((1,), (1,)), ((), ())), preferred_element_type=F32)
            phi = 0.5 * (1.0 + lax.erf(h * 0.7071067811865476))
            act[ps, 0:w] = (h * phi).astype(BF16)
            e = jnp.exp(-0.5 * h * h) * 0.3989422804014327
            gh[ps, fs] = (ga * (phi + h * e)).astype(BF16)

    def put(c, slot, value):
        w, rows = CHUNKS[c] // 2, value.shape[0]
        for n in range(1024 // rows):
            G[c][slot, n * rows : (n + 1) * rows, :] = value[:, n * w : (n + 1) * w]

    def mlp_down(c):
        put(c, core, lax.dot_general(
            act[:, 0 : CHUNKS[c]], cbuf[...], (((0,), (0,)), ((), ())), preferred_element_type=F32))

    def mlp_up(c):
        fs = slice(STARTS[c], STARTS[c] + CHUNKS[c])
        put(c, 1 - core, lax.dot_general(
            sc[...], gh[:, fs], (((0,), (0,)), ((), ())), preferred_element_type=F32))

    def mlp_back(q):
        ps = slice(q * 256, q * 256 + 256)
        gs[ps, :] = lax.dot_general(gh[ps, :], wup[...], (((1,), (1,)), ((), ())), preferred_element_type=F32)

    def blocks(fn):
        @pl.loop(0, 8)
        def _(t):
            fn(t // 2, pl.ds((t % 2) * 8, 8), pl.ds(pl.multiple_of(t * 128, 128), 128))

    def place(c):
        axis = axis_of(c)
        return axis, axis[0] * x + axis[1] * y + axis[2] * z

    def send(c, n, src, dst, to):
        remote(src, dst, csem.at[c, n], rsem.at[c, n], to).start()

    def arrived(c, n, ref):
        landed(ref, rsem.at[c, n])

    def ch_core(c):
        def go(a, n, rows):
            csend[c][a, n] = G[c][1, rows, :].reshape(8, 16, CHUNKS[c] // 2).astype(BF16)
        blocks(go)
        send(c, R_CORE, csend[c], crecv[c], partner)

    def ch_axis(c):
        arrived(c, R_CORE, crecv[c])
        axis, p = place(c)
        def go(a, n, rows):
            M[c][a, n] = (
                G[c][0, rows, :].reshape(8, 16, CHUNKS[c] // 2) + crecv[c][a, n].astype(F32)
            ).astype(BF16)
        blocks(go)
        if direct(c):
            for d in (2, 1, 3):
                send(c, R_A0, M[c].at[(p + d) % 4], axb[c].at[d - 1], along(axis, d))
        else:
            far = (p + 2) % 4
            send(c, R_A0, M[c].at[far, 0:8], axa[c].at[0], along(axis, 1))
            send(c, R_A1, M[c].at[far, 8:16], axa[c].at[1], along(axis, 3))

    def ch_axis2(c):
        axis, p = place(c)
        arrived(c, R_A0, axa[c].at[0])
        arrived(c, R_A1, axa[c].at[1])
        right, left = (p + 1) % 4, (p + 3) % 4
        axs[c][0, 0:8] = (M[c][right, 0:8].astype(F32) + axa[c][0].astype(F32)).astype(BF16)
        axs[c][0, 8:16] = M[c][right, 8:16]
        send(c, R_B0, axs[c].at[0], axb[c].at[0], along(axis, 1))
        axs[c][1, 0:8] = M[c][left, 0:8]
        axs[c][1, 8:16] = (M[c][left, 8:16].astype(F32) + axa[c][1].astype(F32)).astype(BF16)
        send(c, R_B1, axs[c].at[1], axb[c].at[1], along(axis, 3))

    def ch_plane(c):
        axis, p = place(c)
        if direct(c):
            arrived(c, R_A0, axb[c])
        else:
            arrived(c, R_B0, axb[c].at[0])
            arrived(c, R_B1, axb[c].at[1])
        total = M[c][p].astype(F32)
        for n in range(3 if direct(c) else 2):
            total = total + axb[c][n].astype(F32)
        pls[c][...] = total.astype(BF16)

        @pl.loop(1, 16, unroll=5)
        def _(d):
            to, pos = plane_peer(d, axis)
            send(c, R_PRS, pls[c].at[pos], plr[c].at[d - 1], to)

    def ch_share(c):
        axis, p = place(c)
        pos = plane_pos(axis)
        arrived(c, R_PRS, plr[c])
        total = pls[c][pos].astype(F32)
        for d in range(15):
            total = total + plr[c][d].astype(F32)
        GA[c][p, pos] = total.astype(BF16)

        @pl.loop(1, 16, unroll=5)
        def _(d):
            to, _ = plane_peer(d, axis)
            send(c, R_PAG, GA[c].at[p, pos], GA[c].at[p, pos], to)

    def ch_back(c):
        axis, p = place(c)
        arrived(c, R_PAG, plr[c])
        if direct(c):
            for d in (2, 1, 3):
                send(c, R_G0, GA[c].at[p], GA[c].at[p], along(axis, d))
        else:
            send(c, R_G0, GA[c].at[p], GA[c].at[p], along(axis, 1))
            send(c, R_G1, GA[c].at[p], GA[c].at[p], along(axis, 3))
        send(c, R_CAG, GA[c].at[p], GB[c].at[p], partner)

    def ch_back2(c):
        axis, p = place(c)
        right, left = (p + 1) % 4, (p + 3) % 4
        arrived(c, R_G0, GA[c].at[left])
        arrived(c, R_G1, GA[c].at[right])
        a, b = GA[c].at[left, 0:8], GA[c].at[right, 8:16]
        send(c, R_H0, a, a, along(axis, 1))
        send(c, R_H1, b, b, along(axis, 3))
        for q in (left, right):
            send(c, R_CAG, GA[c].at[q], GB[c].at[q], partner)

    def ch_pair(c):
        axis, p = place(c)
        if direct(c):
            arrived(c, R_G0, axb[c])
            for d in (1, 2, 3):
                q = (p + d) % 4
                send(c, R_CAG, GA[c].at[q], GB[c].at[q], partner)
        else:
            arrived(c, R_H0, axa[c].at[0])
            arrived(c, R_H1, axa[c].at[1])
            far = (p + 2) % 4
            send(c, R_CAG, GA[c].at[far], GB[c].at[far], partner)

    def ch_end(c):
        arrived(c, R_CAG, GB[c])

    def ln_back(quarter):
        def body(t, part):
            ps = slice(quarter * 256 + t * 64, quarter * 256 + t * 64 + 64)
            inv = invb[ps, :]
            ns = [nv[cc, ps, :] for cc in range(4)]
            gv = [gs[ps, cc * 128 : cc * 128 + 128] for cc in range(4)]
            prod = [g * n for g, n in zip(gv, ns)]
            part = tuple(
                q + jnp.sum(pr.reshape(8, 8, 128), axis=0) for q, pr in zip(part, prod)
            )
            gains = [gainb[:, cc * 128 : cc * 128 + 128] for cc in range(4)]
            gn = [g * k for g, k in zip(gv, gains)]
            gm = [pr * k for pr, k in zip(prod, gains)]
            m1 = jnp.sum(gn[0] + gn[1] + gn[2] + gn[3], axis=1, keepdims=True) * (1.0 / CH)
            m2 = jnp.sum(gm[0] + gm[1] + gm[2] + gm[3], axis=1, keepdims=True) * (1.0 / CH)
            r, c0 = 2 * quarter + t // 2, (t % 2) * 64
            for cc in range(4):
                g = (inv * (gn[cc] - m1 - ns[cc] * m2)).astype(BF16)
                gb[r, c0 : c0 + 64, cc * 128 : cc * 128 + 128] = g
                gp[cc, 3 + r, LEFT + c0 : LEFT + c0 + 64, :] = g.astype(F32)
            return part

        part = tuple(jnp.zeros((8, 128), F32) for _ in range(4))
        for t in range(4):
            part = body(t, part)
        for cc in range(4):
            row = jnp.sum(part[cc], axis=0, keepdims=True)
            gd[cc, 49:50, :] = row if quarter == 0 else gd[cc, 49:50, :] + row

    back = halo_copies(1, gb)

    def send_back():
        edges(gp, 1)
        for n in (2, 3, 4, 5, 6, 7):
            back[n][0].start()

    def send_rows(k):
        back[0][k].start()
        back[1][k].start()

    def gdw(cc, js):
        @pl.loop(js[0], js[1])
        def _(j):
            def body(cb, acc):
                acc = list(acc)
                base = cb * 64
                for b in range(8):
                    gv = [gp[cc, 3 + r, pl.ds(pl.multiple_of(base + LEFT + 8 * b, 8), 8), :] for r in range(8)]
                    for rho in range(14):
                        v = xf[cc, rho, pl.ds(base + (8 * b + LEFT - 3) + j, 8), :]
                        for r in range(max(0, rho - 6), min(8, rho + 1)):
                            acc[rho - r] = acc[rho - r] + v * gv[r]
                return tuple(acc)

            acc = lax.fori_loop(0, 2, body, tuple(jnp.zeros((8, 128), F32) for _ in range(7)))
            for i in range(7):
                gd[cc, pl.ds(7 * i + j, 1), :] = jnp.sum(acc[i], axis=0, keepdims=True)

    zaxis = (0, 0, 1)
    mine = (x * 4 + y) * 2 + core

    def sm_scatter():
        for cc in range(4):
            for tb in range(8):
                dsm[8 * cc + tb] = gd[cc, 8 * tb : 8 * tb + 8, :]

        @pl.loop(1, 32)
        def _(d):
            to, pos = pair_peer(d)
            remote(dsm.at[pos], dpr.at[d - 1], ssend.at[0], srecv.at[0], to).start()

    def sm_axis():
        landed(dpr, srecv.at[0])
        total = dsm[mine]
        for d in range(31):
            total = total + dpr[d]
        dax[z] = total
        for step in (2, 1, 3):
            remote(dax.at[z], dax.at[z], ssend.at[1], srecv.at[1], along(zaxis, step)).start()

    def sm_share():
        landed(dpr.at[0:3], srecv.at[1])
        dga[mine] = dax[0] + dax[1] + dax[2] + dax[3]

        @pl.loop(1, 32)
        def _(d):
            to, _ = pair_peer(d)
            remote(dga.at[mine], dga.at[mine], ssend.at[2], srecv.at[2], to).start()

    def sm_end():
        landed(dpr, srecv.at[2])
        for cc in range(4):
            for tb in range(8):
                dout[8 * tb : 8 * tb + 8, cc * 128 : cc * 128 + 128] = dga[8 * cc + tb]

    def gin_inner(cb, half):
        @pl.loop(2 * half, 2 * half + 2)
        def _(t):
            conv(gp, True, t, cb, True)

    def gin_outer(cb):
        @pl.loop(0, 4)
        def _(t):
            conv(gp, True, t, cb, False)

    def gin_store(part):
        @pl.loop(part * 8, part * 8 + 8)
        def _(t):
            ps = pl.ds(pl.multiple_of(t * 64, 64), 64)
            for cc in range(4):
                cs = slice(cc * 128, cc * 128 + 128)
                obuf[ps, cs] = (cbuf[ps, cs].astype(F32) + cv[cc, ps, :]).astype(BF16)

    def norm_a():
        for q in range(5):
            if q < 4:
                norm(q)
            if q > 0:
                mlp_a(0, (q - 1,))

    work = []
    chains = {}
    for c, w in enumerate(CHUNKS):
        k = w / 512
        if c == 0:
            work += [(3.0, "norm_a", norm_a, None)]
        else:
            work += [(0.75 * k, "mlp_a", lambda c=c, p=p: mlp_a(c, p), None) for p in ((0, 1), (2, 3))]
        if c == 1:
            work += [(0.01, "last_round", last_round, None)]
        work += [(0.73 * k, "mlp_down", lambda c=c: mlp_down(c), None), (0.73 * k, "mlp_up", lambda c=c: mlp_up(c), c)]
        if direct(c):
            steps = (
                (0.0, ch_core), (2.2, ch_axis), (5.0 + 2.0 * k, ch_plane), (7.0, ch_share), (6.0, ch_back), (6.0, ch_pair), (2.5, ch_end)
            )
        else:
            steps = (
                (0.0, ch_core), (2.5, ch_axis), (4.0, ch_axis2), (5.0, ch_plane), (7.0, ch_share),
                (6.0, ch_back), (5.0, ch_back2), (5.0, ch_pair), (2.5, ch_end),
            )
        chains[c] = [((0.85 if n < 4 else 0.85) * gap, fn.__name__, lambda fn=fn, c=c: fn(c)) for n, (gap, fn) in enumerate(steps)]
    def both(q):
        if q < 4:
            mlp_back(q)
        if q > 0:
            ln_back(q - 1)

    work += [(0.73, "back", lambda q=q: both(q), None) for q in range(5)]
    work += [(0.1, "send_back", send_back, None)]
    small = len(CHUNKS)
    for cc in range(4):
        work += [(0.8, "gdw", lambda cc=cc: gdw(cc, (0, 3)), None)]
        work += [(0.02, "send_rows", lambda cc=cc: send_rows(cc), None)]
        work += [(0.55, "gdw", lambda cc=cc: gdw(cc, (3, 5)), None)]
        work += [(0.55, "gdw", lambda cc=cc: gdw(cc, (5, 7)), small if cc == 3 else None)]
    steps = ((0.0, sm_scatter), (4.6, sm_axis), (3.6, sm_share), (6.0, sm_end))
    chains[small] = [(gap, fn.__name__, fn) for gap, fn in steps]
    for n, cb in enumerate((1, 2, 0, 3)):
        if n == 2:
            work += [(0.05, "halo_c", lambda: halo_cols(1, gp), None)]
        work += [(0.85, "gin_in", lambda cb=cb, half=half: gin_inner(cb, half), None) for half in (0, 1)]
    work += [(0.15, "halo_r", lambda: halo_rows(1, gp), None)]
    work += [(0.7, "gin_out", lambda cb=cb: gin_outer(cb), None) for cb in range(4)]
    work += [(0.2, "gin_st", lambda: gin_store(0), None), (0.2, "gin_st", lambda: gin_store(1), None)]

    now = 0.0
    due = []

    def serve(limit):
        nonlocal now
        while due and (limit is None or min(due)[0] <= limit):
            when, key, n = min(due)
            due.remove((when, key, n))
            now = max(now, when) + 0.1
            with jax.named_scope(f"{chains[key][n][1]}_{key}"):
                chains[key][n][2]()
            if n + 1 < len(chains[key]):
                due.append((now + chains[key][n + 1][0], key, n + 1))

    def drain(chunks, steps):
        for c in chunks:
            sent = [(R_CORE, csend[c]), (R_PRS, plr[c]), (R_PAG, plr[c]), (R_CAG, GA[c])]
            if direct(c):
                sent += [(R_A0, axb[c]), (R_G0, axb[c])]
            else:
                sent += [(R_A0, axa[c].at[0]), (R_A1, axa[c].at[1]), (R_B0, axb[c].at[0]), (R_B1, axb[c].at[1])]
                sent += [(R_G0, axb[c].at[0]), (R_G1, axb[c].at[1]), (R_H0, axa[c].at[0]), (R_H1, axa[c].at[1])]
            for n, ref in sent:
                if n in steps:
                    landed(ref, csem.at[c, n])

    def early_drain():
        for phase in (0, 1):
            for n in range(8):
                buf = hrow.at[phase, n] if n < 2 else hcol.at[phase, n - 2] if n < 4 else hcor.at[phase, n - 4]
                landed(buf, hsend.at[phase, n])
        drain(range(len(CHUNKS)), (R_CORE, R_A0, R_A1, R_B0, R_B1, R_PRS, R_PAG))
        landed(dpr, ssend.at[0])
        landed(dpr.at[0:3], ssend.at[1])

    for cost, name, fn, opens in work:
        with jax.named_scope(name):
            fn()
        now += cost
        if opens is not None:
            due.append((now, opens, 0))
        serve(now)
    with jax.named_scope("early"):
        early_drain()
    serve(None)

    with jax.named_scope("drain"):
        drain(range(len(CHUNKS)), (R_G0, R_G1, R_H0, R_H1, R_CAG))
        landed(dpr, ssend.at[2])


def finish_kernel(*refs):
    refs = list(refs)
    n_ch = len(CHUNKS)
    gin, small = refs[:2]
    own, other = refs[2 : 2 + n_ch], refs[2 + n_ch : 2 + 2 * n_ch]
    gout_hbm, dw_hbm, gain_hbm, up_hbm, down_hbm, dbuf, kbuf = refs[2 + 2 * n_ch : 9 + 2 * n_ch]
    downs, ups = refs[9 + 2 * n_ch : 9 + 3 * n_ch], refs[9 + 3 * n_ch : 9 + 4 * n_ch]
    osem = refs[-1]
    outs = []

    def put(src, dst):
        outs.append(pltpu.make_async_copy(src, dst, osem.at[len(outs)]))
        outs[-1].start()

    def widen(c, down, up):
        half = CHUNKS[c] // 2
        for narrow, wide in ((down, downs[c]), (up, ups[c])):
            rows = wide.shape[0]
            step = rows // 4

            @pl.loop(0, 4)
            def _(t):
                rs = pl.ds(pl.multiple_of(t * step, step), step)
                for n in range(1024 // rows):
                    wide[rs, n * half : (n + 1) * half] = narrow[
                        pl.ds(pl.multiple_of(n * rows + t * step, step), step), :
                    ].astype(F32)

    core = lax.axis_index("rows") % 2
    for c, w in enumerate(CHUNKS):
        @pl.when(core == 0)
        def _():
            widen(c, own[c], other[c])

        @pl.when(core == 1)
        def _():
            widen(c, other[c], own[c])

        part = pl.ds(STARTS[c], w)
        put(downs[c], down_hbm.at[part])
        put(ups[c], up_hbm.at[:, part])
    put(gin, gout_hbm)
    dbuf[...] = small[0:49, :]
    kbuf[...] = small[49:50, :]
    put(dbuf, dw_hbm)
    put(kbuf, gain_hbm)
    for c_ in outs:
        c_.wait()


def finish(gin, small, big):
    vm, dma = pltpu.VMEM, pltpu.SemaphoreType.DMA
    any_, here = pl.BlockSpec(memory_space=pl.ANY), pl.BlockSpec(memory_space=pltpu.VMEM)
    n_ch = len(CHUNKS)
    gin, dw, gain, up, down = pl.pallas_call(
        finish_kernel,
        out_shape=(
            jax.ShapeDtypeStruct((PIX, CH), BF16),
            jax.ShapeDtypeStruct((49, CH), F32),
            jax.ShapeDtypeStruct((1, CH), F32),
            jax.ShapeDtypeStruct((CH, FF), F32),
            jax.ShapeDtypeStruct((FF, CH), F32),
        ),
        in_specs=[here] * (2 + 2 * n_ch),
        out_specs=[any_] * 5,
        scratch_shapes=[vm((49, CH), F32), vm((1, CH), F32)]
        + [vm((w, CH), F32) for w in CHUNKS]
        + [vm((CH, w), F32) for w in CHUNKS]
        + [dma((2 * n_ch + 3,))],
        compiler_params=pltpu.CompilerParams(vmem_limit_bytes=24_000_000),
        name="finish",
    )(gin, small, *[b.reshape(1024, w // 2) for b, w in zip(big, CHUNKS * 2)])
    return gin.reshape(ROWS, COLS, CH), dw, gain.reshape(CH), up, down


def on_device(features, dw_weight, norm_gain, w_up, w_down, cotangent):
    vm, dma = pltpu.VMEM, pltpu.SemaphoreType.DMA
    any_ = pl.BlockSpec(memory_space=pl.ANY)
    n_ch = len(CHUNKS)
    comm = []
    for c, w in enumerate(CHUNKS):
        h = w // 2
        whole = vm((4, 16, 16, h), BF16)
        comm += [vm((2, 1024, h), F32), whole, whole, whole]
        comm += [vm((2, 8, 16, h), BF16), vm((2, 16, 16, h), BF16), vm((3 if direct(c) else 2, 16, 16, h), BF16)]
        comm += [vm((16, 16, h), BF16), vm((15, 16, h), BF16)]
    gin, small, *big = pl.pallas_call(
        kernel,
        out_shape=(
            vm((PIX, CH), BF16),
            vm((64, CH), F32),
            *[vm((4, 16, 16, w // 2), BF16) for w in CHUNKS * 2],
        ),
        in_specs=[any_] * 6,
        out_specs=[pl.BlockSpec(memory_space=pltpu.VMEM)] * (2 + 2 * n_ch),
        scratch_shapes=[
            vm((ROWS, COLS, CH), BF16), vm((PIX, CH), BF16), vm((CH, FF), BF16), vm((FF, CH), BF16),
            vm((49, CH), F32), vm((1, CH), F32),
            vm((4, 14, 144, 128), F32), vm((4, 14, 144, 128), F32), vm((4, 49, 8, 128), F32),
            vm((4, PIX, 128), F32), vm((4, PIX, 128), F32), vm((PIX, 128), F32), vm((PIX, CH), BF16),
            vm((PIX, max(CHUNKS)), BF16), vm((PIX, FF), BF16), vm((PIX, CH), F32),
            vm((ROWS, COLS, CH), BF16),
            vm((2, 2, 8, 8, CH), BF16), vm((2, 2, 3, COLS, CH), BF16), vm((2, 2, 8, 8, CH), BF16), vm((2, 4, 3, 8, CH), BF16),
            vm((4, 64, 128), F32), vm((32, 8, 128), F32), vm((31, 8, 128), F32), vm((4, 8, 128), F32),
            vm((32, 8, 128), F32),
        ]
        + comm
        + [
            dma((6,)), dma((2, 8)), dma((2, 8)), dma((n_ch, 12)), dma((n_ch, 12)), dma((3,)), dma((3,)),
            pltpu.SemaphoreType.REGULAR((4,)),
        ],
        compiler_params=pltpu.CompilerParams(
            collective_id=0, has_side_effects=True, vmem_limit_bytes=58_000_000
        ),
        name="block_backward",
    )(features, dw_weight, norm_gain.reshape(1, CH), w_up, w_down, cotangent.reshape(PIX, CH))
    return finish(gin, small, big)


def solution(mesh):
    return jax.shard_map(
        on_device,
        mesh=mesh,
        in_specs=(P("rows", "cols", None), P(), P(), P(), P(), P("rows", "cols", None)),
        out_specs=(P("rows", "cols", None), P(), P(), P(), P()),
        check_vma=False,
    )
```

```python
import jax
import jax.numpy as jnp
from jax import lax
from jax.experimental import pallas as pl
from jax.experimental.pallas import tpu as pltpu
from jax.sharding import PartitionSpec as P

EPS = 1e-06
ROWS, COLS, CH, FF = 8, 128, 512, 2048
PIX = ROWS * COLS
CHUNKS = (512, 512, 512, 256, 256)
STARTS = tuple(sum(CHUNKS[:n]) for n in range(len(CHUNKS)))
LEFT = 8
F32, BF16 = jnp.float32, jnp.bfloat16
MESH = pl.DeviceIdType.MESH
FIRST_AXIS = ((0, 2), (1, 0), (2, 1), (0, 2), (2, 0))
SIDES = ((-1, 0), (1, 0), (0, -1), (0, 1), (-1, -1), (-1, 1), (1, -1), (1, 1))
(R_CORE, R_A0, R_A1, R_B0, R_B1, R_PRS, R_PAG, R_G0, R_G1, R_H0, R_H1, R_CAG) = range(12)


def direct(c):
    return c > 1


def kernel(*refs):
    refs = list(refs)

    def take(n):
        out = refs[:n]
        del refs[:n]
        return out

    feat_hbm, dww_hbm, gain_hbm, wup_hbm, wdn_hbm, cot_hbm = take(6)
    obuf, dout = take(2)
    GA, GB = take(len(CHUNKS)), take(len(CHUNKS))
    fbuf, cbuf, wup, wdn, dww, gainb, xf, gp, wb, cv, nv, invb, sc, sct = take(14)
    act, gh, gs, gb, scol, hrow, hcol, hcor = take(8)
    gd, dsm, dpr, dax, dga = take(5)
    G, csend, crecv, M, axa, axs, axb, pls, plr = zip(*[take(9) for _ in CHUNKS])
    ld, hsend, hrecv, csem, rsem, ssend, srecv, near = take(8)

    ra, ca = lax.axis_index("rows"), lax.axis_index("cols")
    core = ra % 2
    y, z, x = (ra // 2) % 4, ra // 8, ca

    def device(x_, y_, z_, core_):
        return ((z_ * 4 + y_) * 2 + core_, x_)

    partner = device(x, y, z, 1 - core)

    def side(dr, dc):
        return ((ra + dr + 32) % 32, (ca + dc + 4) % 4)

    def plane_peer(d, axis):
        ix, iy, iz = axis
        u, v = ix * y + iy * z + iz * x, ix * z + iy * x + iz * y
        u2, v2 = (u + d // 4) % 4, (v + d % 4) % 4
        return (
            device(
                ix * x + iy * v2 + iz * u2,
                ix * u2 + iy * y + iz * v2,
                ix * v2 + iy * u2 + iz * z,
                core,
            ),
            u2 * 4 + v2,
        )

    def plane_pos(axis):
        ix, iy, iz = axis
        return (ix * y + iy * z + iz * x) * 4 + ix * z + iy * x + iz * y

    def pair_peer(d):
        x2, y2, core2 = (x + d // 8) % 4, (y + (d // 2) % 4) % 4, (core + d % 2) % 2
        return device(x2, y2, z, core2), (x2 * 4 + y2) * 2 + core2

    def axis_of(c):
        a0, a1 = FIRST_AXIS[c]
        return tuple((a0 == n) * (1 - core) + (a1 == n) * core for n in range(3))

    def along(axis, step):
        ix, iy, iz = axis
        return device(
            (x + step * ix) % 4, (y + step * iy) % 4, (z + step * iz) % 4, core
        )

    def remote(src, dst, send, recv, to):
        return pltpu.make_async_remote_copy(
            src_ref=src, dst_ref=dst, send_sem=send, recv_sem=recv, device_id=to, device_id_type=MESH
        )

    def landed(ref, sem):
        pltpu.make_async_copy(ref, ref, sem).wait()

    loads = [
        pltpu.make_async_copy(s, d, ld.at[n])
        for n, (s, d) in enumerate(
            ((feat_hbm, fbuf), (dww_hbm, dww), (gain_hbm, gainb), (cot_hbm, cbuf), (wup_hbm, wup), (wdn_hbm, wdn))
        )
    ]
    for c_ in loads:
        c_.start()
    barrier = pltpu.get_barrier_semaphore()
    for dr, dc in SIDES:
        pl.semaphore_signal(barrier, inc=1, device_id=side(dr, dc), device_id_type=MESH)

    NEAR = [along(tuple(int(n == k) for n in range(3)), step) for k in range(3) for step in (1, 3)]
    for to in NEAR:
        pl.semaphore_signal(barrier, inc=1, device_id=to, device_id_type=MESH)

    def round_signal(n):
        for to in [partner] + NEAR:
            pl.semaphore_signal(near.at[n], inc=1, device_id=to, device_id_type=MESH)

    def round_wait(n):
        pl.semaphore_wait(near.at[n], 1 + len(NEAR))

    for c_ in loads[:3]:
        c_.wait()

    def edges(pad, phase):
        for n, start in ((0, LEFT), (1, LEFT + COLS - 8)):
            for cc in range(4):
                scol[phase, n, :, :, cc * 128 : cc * 128 + 128] = pad[
                    cc, 3 : 3 + ROWS, start : start + 8, :
                ].astype(BF16)

    with jax.named_scope("widen"):
        @pl.loop(0, ROWS)
        def _(r):
            for cc in range(4):
                xf[cc, 3 + r, LEFT : LEFT + COLS, :] = fbuf[r, :, cc * 128 : cc * 128 + 128].astype(F32)

        edges(xf, 0)
        for cc in range(4):
            gd[cc, 48:64, :] = jnp.zeros((16, 128), F32)

    with jax.named_scope("entry"):
        pl.semaphore_wait(barrier, len(SIDES) + len(NEAR))
        round_signal(0)

    def halo_copies(phase, rows_src):
        out = []
        for n, (dr, dc) in enumerate(SIDES):
            rs = slice(0, 3) if dr < 0 else slice(5, 8)
            if dc == 0:
                src, dst = rows_src.at[rs], hrow.at[phase, n]
            elif dr == 0:
                src, dst = scol.at[phase, n - 2], hcol.at[phase, n - 2]
            else:
                src, dst = scol.at[phase, 0 if dc < 0 else 1, rs], hcor.at[phase, n - 4]
            if dc == 0 and phase == 1:
                cols = [pl.ds(32 * k, 32) for k in range(4)]
                out.append([
                    remote(src.at[:, k], dst.at[:, k], hsend.at[1, n], hrecv.at[1, n], side(dr, dc)) for k in cols
                ])
            else:
                out.append([remote(src, dst, hsend.at[phase, n], hrecv.at[phase, n], side(dr, dc))])
        return out

    def halo_landed(phase, n):
        buf = hrow.at[phase, n] if n < 2 else hcol.at[phase, n - 2] if n < 4 else hcor.at[phase, n - 4]
        landed(buf, hrecv.at[phase, n])

    valid = {
        -1: jnp.where(ra < 31, 1.0, 0.0).astype(F32),
        1: jnp.where(ra > 0, 1.0, 0.0).astype(F32),
    }
    valid_c = {
        -1: jnp.where(ca < 3, 1.0, 0.0).astype(F32),
        1: jnp.where(ca > 0, 1.0, 0.0).astype(F32),
    }

    def halo_cols(phase, pad):
        for n in (2, 3):
            halo_landed(phase, n)
            dc = SIDES[n][1]
            start = LEFT + COLS if dc < 0 else LEFT - 8
            for cc in range(4):
                pad[cc, 3 : 3 + ROWS, start : start + 8, :] = (
                    hcol[phase, n - 2, :, :, cc * 128 : cc * 128 + 128].astype(F32) * valid_c[dc]
                )

    def halo_rows(phase, pad):
        for n in (0, 1):
            halo_landed(phase, n)
            dr = SIDES[n][0]
            r0 = 3 + ROWS if dr < 0 else 0
            for r in range(3):
                for cc in range(4):
                    pad[cc, r0 + r, LEFT : LEFT + COLS, :] = (
                        hrow[phase, n, r, :, cc * 128 : cc * 128 + 128].astype(F32) * valid[dr]
                    )
        for n in range(4, 8):
            halo_landed(phase, n)
            dr, dc = SIDES[n]
            r0 = 3 + ROWS if dr < 0 else 0
            start = LEFT + COLS if dc < 0 else LEFT - 8
            for cc in range(4):
                pad[cc, r0 : r0 + 3, start : start + 8, :] = hcor[
                    phase, n - 4, :, :, cc * 128 : cc * 128 + 128
                ].astype(F32) * (valid[dr] * valid_c[dc])

    def conv(pad, flip, cc, starts, inner):
        rhos = range(3, 11) if inner else (0, 1, 2, 11, 12, 13)
        rows = range(ROWS) if inner else (0, 1, 2, 5, 6, 7)

        def at(r, b):
            return pl.ds(pl.multiple_of(r * COLS + starts[b], 8), 8)

        def body(j, acc):
            acc = dict(zip([(r, b) for r in rows for b in range(4)], acc))
            w = [wb[cc, (48 - 7 * i - j) if flip else (7 * i + j)] for i in range(7)]
            for rho in rhos:
                for b in range(4):
                    v = pad[cc, rho, pl.ds(starts[b] + (LEFT - 3) + j, 8), :]
                    for r in rows:
                        if 0 <= rho - r <= 6:
                            acc[r, b] = acc[r, b] + v * w[rho - r]
            return tuple(acc.values())

        if inner:
            start = tuple(jnp.zeros((8, 128), F32) for r in rows for b in range(4))
        else:
            start = tuple(cv[cc, at(r, b), :] for r in rows for b in range(4))
        acc = lax.fori_loop(0, 7, body, start, unroll=7)
        for n, (r, b) in enumerate([(r, b) for r in rows for b in range(4)]):
            cv[cc, at(r, b), :] = acc[n]

    def groups(base):
        return [base + 8 * b for b in range(4)]

    halo = halo_copies(0, fbuf)
    with jax.named_scope("taps"):
        for n in (2, 3, 0, 1, 4, 5, 6, 7):
            halo[n][0].start()

        for t in range(49):
            for cc in range(4):
                wb[cc, t] = jnp.broadcast_to(dww[t : t + 1, cc * 128 : cc * 128 + 128], (8, 128))

    with jax.named_scope("fconv_mid"):
        @pl.loop(0, 12)
        def _(t):
            conv(xf, False, t // 3, groups(8 + 32 * (t % 3)), True)

    with jax.named_scope("fhalo_c"):
        round_wait(0)
        round_signal(1)
        halo_cols(0, xf)

    with jax.named_scope("fconv_side"):
        @pl.loop(0, 4)
        def _(t):
            conv(xf, False, t, (0, 104, 112, 120), True)

    with jax.named_scope("fhalo_r"):
        round_wait(1)
        round_signal(2)
        halo_rows(0, xf)

    with jax.named_scope("fconv_out"):
        @pl.loop(0, 16)
        def _(t):
            conv(xf, False, t // 4, groups(32 * (t % 4)), False)

    round_wait(2)
    round_signal(3)

    def norm(quarter):
        for t in range(4):
            ps = slice(quarter * 256 + t * 64, quarter * 256 + t * 64 + 64)
            v = [cv[cc, ps, :] for cc in range(4)]
            mean = jnp.sum(v[0] + v[1] + v[2] + v[3], axis=1, keepdims=True) * (1.0 / CH)
            v = [a - mean for a in v]
            sq = [a * a for a in v]
            inv = lax.rsqrt(jnp.sum(sq[0] + sq[1] + sq[2] + sq[3], axis=1, keepdims=True) * (1.0 / CH) + EPS)
            invb[ps, :] = jnp.broadcast_to(inv, (64, 128))
            for cc in range(4):
                n_ = v[cc] * inv
                nv[cc, ps, :] = n_
                sc[ps, cc * 128 : cc * 128 + 128] = (n_ * gainb[:, cc * 128 : cc * 128 + 128]).astype(BF16)

    for c_ in loads[3:]:
        c_.wait()

    def last_round():
        round_wait(3)

    def mlp_a(c, pbs):
        w = CHUNKS[c]
        fs = slice(STARTS[c], STARTS[c] + w)
        for pb in pbs:
            ps = slice(pb * 256, pb * 256 + 256)
            h = jnp.dot(sc[ps, :], wup[:, fs], preferred_element_type=F32)
            ga = lax.dot_general(cbuf[ps, :], wdn[fs, :], (((1,), (1,)), ((), ())), preferred_element_type=F32)
            phi = 0.5 * (1.0 + lax.erf(h * 0.7071067811865476))
            act[ps, 0:w] = (h * phi).astype(BF16)
            e = jnp.exp(-0.5 * h * h) * 0.3989422804014327
            gh[ps, fs] = (ga * (phi + h * e)).astype(BF16)

    def put(c, slot, value):
        w, rows = CHUNKS[c] // 2, value.shape[0]
        for n in range(1024 // rows):
            G[c][slot, n * rows : (n + 1) * rows, :] = value[:, n * w : (n + 1) * w]

    def mlp_down(c):
        put(c, core, lax.dot_general(
            act[:, 0 : CHUNKS[c]], cbuf[...], (((0,), (0,)), ((), ())), preferred_element_type=F32))

    def mlp_up(c):
        fs = slice(STARTS[c], STARTS[c] + CHUNKS[c])
        if CHUNKS[c] < 512:
            for n in range(2):
                rs = slice(n * 256, n * 256 + 256)
                v = jnp.dot(sct[rs, :], gh[:, fs], preferred_element_type=F32)
                w = CHUNKS[c] // 2
                for k in range(2):
                    G[c][1 - core, k * 512 + n * 256 : k * 512 + n * 256 + 256, :] = v[:, k * w : (k + 1) * w]
        else:
            put(c, 1 - core, jnp.dot(sct[...], gh[:, fs], preferred_element_type=F32))

    def mlp_back(q):
        ps = slice(q * 256, q * 256 + 256)
        gs[ps, :] = lax.dot_general(gh[ps, :], wup[...], (((1,), (1,)), ((), ())), preferred_element_type=F32)

    def blocks(fn):
        @pl.loop(0, 8)
        def _(t):
            fn(t // 2, pl.ds((t % 2) * 8, 8), pl.ds(pl.multiple_of(t * 128, 128), 128))

    def place(c):
        axis = axis_of(c)
        return axis, axis[0] * x + axis[1] * y + axis[2] * z

    def send(c, n, src, dst, to):
        remote(src, dst, csem.at[c, n], rsem.at[c, n], to).start()

    def arrived(c, n, ref):
        landed(ref, rsem.at[c, n])

    def ch_core(c):
        def go(a, n, rows):
            csend[c][a, n] = G[c][1, rows, :].reshape(8, 16, CHUNKS[c] // 2).astype(BF16)
        blocks(go)
        send(c, R_CORE, csend[c], crecv[c], partner)

    def ch_axis(c):
        arrived(c, R_CORE, crecv[c])
        axis, p = place(c)
        def go(a, n, rows):
            M[c][a, n] = (
                G[c][0, rows, :].reshape(8, 16, CHUNKS[c] // 2) + crecv[c][a, n].astype(F32)
            ).astype(BF16)
        blocks(go)
        if direct(c):
            for d in (2, 1, 3):
                send(c, R_A0, M[c].at[(p + d) % 4], axb[c].at[d - 1], along(axis, d))
        else:
            far = (p + 2) % 4
            send(c, R_A0, M[c].at[far, 0:8], axa[c].at[0], along(axis, 1))
            send(c, R_A1, M[c].at[far, 8:16], axa[c].at[1], along(axis, 3))

    def ch_axis2(c):
        axis, p = place(c)
        arrived(c, R_A0, axa[c].at[0])
        arrived(c, R_A1, axa[c].at[1])
        right, left = (p + 1) % 4, (p + 3) % 4
        axs[c][0, 0:8] = (M[c][right, 0:8].astype(F32) + axa[c][0].astype(F32)).astype(BF16)
        axs[c][0, 8:16] = M[c][right, 8:16]
        send(c, R_B0, axs[c].at[0], axb[c].at[0], along(axis, 1))
        axs[c][1, 0:8] = M[c][left, 0:8]
        axs[c][1, 8:16] = (M[c][left, 8:16].astype(F32) + axa[c][1].astype(F32)).astype(BF16)
        send(c, R_B1, axs[c].at[1], axb[c].at[1], along(axis, 3))

    def ch_plane(c):
        axis, p = place(c)
        if direct(c):
            arrived(c, R_A0, axb[c])
        else:
            arrived(c, R_B0, axb[c].at[0])
            arrived(c, R_B1, axb[c].at[1])
        total = M[c][p].astype(F32)
        for n in range(3 if direct(c) else 2):
            total = total + axb[c][n].astype(F32)
        pls[c][...] = total.astype(BF16)

        @pl.loop(1, 16, unroll=15)
        def _(d):
            to, pos = plane_peer(d, axis)
            send(c, R_PRS, pls[c].at[pos], plr[c].at[d - 1], to)

    def ch_share(c):
        axis, p = place(c)
        pos = plane_pos(axis)
        arrived(c, R_PRS, plr[c])
        total = pls[c][pos].astype(F32)
        for d in range(15):
            total = total + plr[c][d].astype(F32)
        GA[c][p, pos] = total.astype(BF16)

        @pl.loop(1, 16, unroll=15)
        def _(d):
            to, _ = plane_peer(d, axis)
            send(c, R_PAG, GA[c].at[p, pos], GA[c].at[p, pos], to)

    def ch_back(c):
        axis, p = place(c)
        arrived(c, R_PAG, plr[c])
        if direct(c):
            for d in (2, 1, 3):
                send(c, R_G0, GA[c].at[p], GA[c].at[p], along(axis, d))
        else:
            send(c, R_G0, GA[c].at[p], GA[c].at[p], along(axis, 1))
            send(c, R_G1, GA[c].at[p], GA[c].at[p], along(axis, 3))
        send(c, R_CAG, GA[c].at[p], GB[c].at[p], partner)

    def ch_back2(c):
        axis, p = place(c)
        right, left = (p + 1) % 4, (p + 3) % 4
        arrived(c, R_G0, GA[c].at[left])
        arrived(c, R_G1, GA[c].at[right])
        a, b = GA[c].at[left, 0:8], GA[c].at[right, 8:16]
        send(c, R_H0, a, a, along(axis, 1))
        send(c, R_H1, b, b, along(axis, 3))
        for q in (left, right):
            send(c, R_CAG, GA[c].at[q], GB[c].at[q], partner)

    def ch_pair(c):
        axis, p = place(c)
        if direct(c):
            arrived(c, R_G0, axb[c])
            for d in (1, 2, 3):
                q = (p + d) % 4
                send(c, R_CAG, GA[c].at[q], GB[c].at[q], partner)
        else:
            arrived(c, R_H0, axa[c].at[0])
            arrived(c, R_H1, axa[c].at[1])
            far = (p + 2) % 4
            send(c, R_CAG, GA[c].at[far], GB[c].at[far], partner)

    def ch_end(c):
        arrived(c, R_CAG, GB[c])

    def ln_back(quarter):
        def body(t, part):
            ps = slice(quarter * 256 + t * 64, quarter * 256 + t * 64 + 64)
            inv = invb[ps, :]
            ns = [nv[cc, ps, :] for cc in range(4)]
            gv = [gs[ps, cc * 128 : cc * 128 + 128] for cc in range(4)]
            prod = [g * n for g, n in zip(gv, ns)]
            part = tuple(
                q + jnp.sum(pr.reshape(8, 8, 128), axis=0) for q, pr in zip(part, prod)
            )
            gains = [gainb[:, cc * 128 : cc * 128 + 128] for cc in range(4)]
            gn = [g * k for g, k in zip(gv, gains)]
            gm = [pr * k for pr, k in zip(prod, gains)]
            m1 = jnp.sum(gn[0] + gn[1] + gn[2] + gn[3], axis=1, keepdims=True) * (1.0 / CH)
            m2 = jnp.sum(gm[0] + gm[1] + gm[2] + gm[3], axis=1, keepdims=True) * (1.0 / CH)
            r, c0 = 2 * quarter + t // 2, (t % 2) * 64
            for cc in range(4):
                g = (inv * (gn[cc] - m1 - ns[cc] * m2)).astype(BF16)
                gb[r, c0 : c0 + 64, cc * 128 : cc * 128 + 128] = g
                gp[cc, 3 + r, LEFT + c0 : LEFT + c0 + 64, :] = g.astype(F32)
            return part

        part = tuple(jnp.zeros((8, 128), F32) for _ in range(4))
        for t in range(4):
            part = body(t, part)
        for cc in range(4):
            row = jnp.sum(part[cc], axis=0, keepdims=True)
            gd[cc, 49:50, :] = row if quarter == 0 else gd[cc, 49:50, :] + row

    back = halo_copies(1, gb)

    def send_back():
        edges(gp, 1)
        for n in (2, 3, 4, 5, 6, 7):
            back[n][0].start()

    def send_rows(k):
        back[0][k].start()
        back[1][k].start()

    def gdw(cc, js):
        @pl.loop(js[0], js[1])
        def _(j):
            def body(cb, acc):
                acc = list(acc)
                base = cb * 64
                for b in range(8):
                    gv = [gp[cc, 3 + r, pl.ds(pl.multiple_of(base + LEFT + 8 * b, 8), 8), :] for r in range(8)]
                    for rho in range(14):
                        v = xf[cc, rho, pl.ds(base + (8 * b + LEFT - 3) + j, 8), :]
                        for r in range(max(0, rho - 6), min(8, rho + 1)):
                            acc[rho - r] = acc[rho - r] + v * gv[r]
                return tuple(acc)

            acc = lax.fori_loop(0, 2, body, tuple(jnp.zeros((8, 128), F32) for _ in range(7)))
            for i in range(7):
                gd[cc, pl.ds(7 * i + j, 1), :] = jnp.sum(acc[i], axis=0, keepdims=True)

    zaxis = (0, 0, 1)
    mine = (x * 4 + y) * 2 + core

    def sm_scatter():
        for cc in range(4):
            for tb in range(8):
                dsm[8 * cc + tb] = gd[cc, 8 * tb : 8 * tb + 8, :]

        @pl.loop(1, 32, unroll=31)
        def _(d):
            to, pos = pair_peer(d)
            remote(dsm.at[pos], dpr.at[d - 1], ssend.at[0], srecv.at[0], to).start()

    def sm_axis():
        landed(dpr, srecv.at[0])
        total = dsm[mine]
        for d in range(31):
            total = total + dpr[d]
        dax[z] = total
        for step in (2, 1, 3):
            remote(dax.at[z], dax.at[z], ssend.at[1], srecv.at[1], along(zaxis, step)).start()

    def sm_share():
        landed(dpr.at[0:3], srecv.at[1])
        dga[mine] = dax[0] + dax[1] + dax[2] + dax[3]

        @pl.loop(1, 32, unroll=31)
        def _(d):
            to, _ = pair_peer(d)
            remote(dga.at[mine], dga.at[mine], ssend.at[2], srecv.at[2], to).start()

    def sm_end():
        landed(dpr, srecv.at[2])
        for cc in range(4):
            for tb in range(8):
                dout[8 * tb : 8 * tb + 8, cc * 128 : cc * 128 + 128] = dga[8 * cc + tb]

    def gin_inner(cb, half):
        @pl.loop(2 * half, 2 * half + 2)
        def _(t):
            conv(gp, True, t, groups(32 * cb), True)

    def gin_outer(cb):
        @pl.loop(0, 4)
        def _(t):
            conv(gp, True, t, groups(32 * cb), False)

    def gin_store(part):
        @pl.loop(part * 8, part * 8 + 8)
        def _(t):
            ps = pl.ds(pl.multiple_of(t * 64, 64), 64)
            for cc in range(4):
                cs = slice(cc * 128, cc * 128 + 128)
                obuf[ps, cs] = (cbuf[ps, cs].astype(F32) + cv[cc, ps, :]).astype(BF16)

    def norm_a():
        for q in range(5):
            if q < 4:
                norm(q)
                qs = slice(q * 256, q * 256 + 256)
                sct[:, qs] = sc[qs, :].T
            if q > 0:
                mlp_a(0, (q - 1,))

    work = []
    chains = {}
    for c, w in enumerate(CHUNKS):
        k = w / 512
        if c == 0:
            work += [(3.0, "norm_a", norm_a, None)]
        else:
            work += [(0.75 * k, "mlp_a", lambda c=c, p=p: mlp_a(c, p), None) for p in ((0, 1), (2, 3))]
        if c == 1:
            work += [(0.01, "last_round", last_round, None)]
        work += [(0.73 * k, "mlp_down", lambda c=c: mlp_down(c), None), (0.73 * k, "mlp_up", lambda c=c: mlp_up(c), c)]
        if direct(c):
            steps = (
                (0.0, ch_core), (2.2, ch_axis), (5.0 + 2.0 * k, ch_plane), (7.0, ch_share), (6.0, ch_back), (6.0, ch_pair), (2.5, ch_end)
            )
        else:
            steps = (
                (0.0, ch_core), (2.5, ch_axis), (4.0, ch_axis2), (5.0, ch_plane), (7.0, ch_share),
                (6.0, ch_back), (5.0, ch_back2), (5.0, ch_pair), (2.5, ch_end),
            )
        more = {(2, ch_back): 1.8}
        steps = tuple((gap + more.get((c, fn), 0.0), fn) for gap, fn in steps)
        chains[c] = [((0.85 if n < 4 else 0.85) * gap, fn.__name__, lambda fn=fn, c=c: fn(c)) for n, (gap, fn) in enumerate(steps)]
    def both(q):
        if q < 4:
            mlp_back(q)
        if q > 0:
            ln_back(q - 1)

    work += [(0.73, "back", lambda q=q: both(q), None) for q in range(5)]
    work += [(0.1, "send_back", send_back, None)]
    small = len(CHUNKS)
    for cc in range(4):
        work += [(0.8, "gdw", lambda cc=cc: gdw(cc, (0, 3)), None)]
        work += [(0.02, "send_rows", lambda cc=cc: send_rows(cc), None)]
        work += [(0.55, "gdw", lambda cc=cc: gdw(cc, (3, 5)), None)]
        work += [(0.55, "gdw", lambda cc=cc: gdw(cc, (5, 7)), small if cc == 3 else None)]
    steps = ((0.0, sm_scatter), (4.6, sm_axis), (3.6, sm_share), (6.0, sm_end))
    chains[small] = [(gap, fn.__name__, fn) for gap, fn in steps]
    for n, cb in enumerate((1, 2, 0, 3)):
        if n == 2:
            work += [(0.05, "halo_c", lambda: halo_cols(1, gp), None)]
        work += [(0.85, "gin_in", lambda cb=cb, half=half: gin_inner(cb, half), None) for half in (0, 1)]
    work += [(0.15, "halo_r", lambda: halo_rows(1, gp), None)]
    work += [(0.7, "gin_out", lambda cb=cb: gin_outer(cb), None) for cb in range(4)]
    work += [(0.2, "gin_st", lambda: gin_store(0), None), (0.2, "gin_st", lambda: gin_store(1), None)]

    now = 0.0
    due = []

    def serve(limit):
        nonlocal now
        while due and (limit is None or min(due)[0] <= limit):
            when, key, n = min(due)
            due.remove((when, key, n))
            now = max(now, when) + 0.1
            with jax.named_scope(f"{chains[key][n][1]}_{key}"):
                chains[key][n][2]()
            if n + 1 < len(chains[key]):
                due.append((now + chains[key][n + 1][0], key, n + 1))

    def drain(chunks, steps):
        for c in chunks:
            sent = [(R_CORE, csend[c]), (R_PRS, plr[c]), (R_PAG, plr[c]), (R_CAG, GA[c])]
            if direct(c):
                sent += [(R_A0, axb[c]), (R_G0, axb[c])]
            else:
                sent += [(R_A0, axa[c].at[0]), (R_A1, axa[c].at[1]), (R_B0, axb[c].at[0]), (R_B1, axb[c].at[1])]
                sent += [(R_G0, axb[c].at[0]), (R_G1, axb[c].at[1]), (R_H0, axa[c].at[0]), (R_H1, axa[c].at[1])]
            for n, ref in sent:
                if n in steps:
                    landed(ref, csem.at[c, n])

    def early_drain():
        for phase in (0, 1):
            for n in range(8):
                buf = hrow.at[phase, n] if n < 2 else hcol.at[phase, n - 2] if n < 4 else hcor.at[phase, n - 4]
                landed(buf, hsend.at[phase, n])
        drain(range(len(CHUNKS)), (R_CORE, R_A0, R_A1, R_B0, R_B1, R_PRS, R_PAG))
        landed(dpr, ssend.at[0])
        landed(dpr.at[0:3], ssend.at[1])

    for cost, name, fn, opens in work:
        with jax.named_scope(name):
            fn()
        now += cost
        if opens is not None:
            due.append((now, opens, 0))
        serve(now)
    with jax.named_scope("early"):
        early_drain()
    serve(None)

    with jax.named_scope("drain"):
        drain(range(len(CHUNKS)), (R_G0, R_G1, R_H0, R_H1, R_CAG))
        landed(dpr, ssend.at[2])


def finish_kernel(*refs):
    refs = list(refs)
    n_ch = len(CHUNKS)
    gin, small = refs[:2]
    own, other = refs[2 : 2 + n_ch], refs[2 + n_ch : 2 + 2 * n_ch]
    gout_hbm, dw_hbm, gain_hbm, up_hbm, down_hbm, dbuf, kbuf = refs[2 + 2 * n_ch : 9 + 2 * n_ch]
    downs, ups = refs[9 + 2 * n_ch : 9 + 3 * n_ch], refs[9 + 3 * n_ch : 9 + 4 * n_ch]
    osem = refs[-1]
    outs = []

    def put(src, dst):
        outs.append(pltpu.make_async_copy(src, dst, osem.at[len(outs)]))
        outs[-1].start()

    def widen(c, down, up):
        half = CHUNKS[c] // 2
        for narrow, wide in ((down, downs[c]), (up, ups[c])):
            rows = wide.shape[0]
            step = rows // 4

            @pl.loop(0, 4)
            def _(t):
                rs = pl.ds(pl.multiple_of(t * step, step), step)
                for n in range(1024 // rows):
                    wide[rs, n * half : (n + 1) * half] = narrow[
                        pl.ds(pl.multiple_of(n * rows + t * step, step), step), :
                    ].astype(F32)

    core = lax.axis_index("rows") % 2
    for c, w in enumerate(CHUNKS):
        @pl.when(core == 0)
        def _():
            widen(c, own[c], other[c])

        @pl.when(core == 1)
        def _():
            widen(c, other[c], own[c])

        part = pl.ds(STARTS[c], w)
        put(downs[c], down_hbm.at[part])
        put(ups[c], up_hbm.at[:, part])
    put(gin, gout_hbm)
    dbuf[...] = small[0:49, :]
    kbuf[...] = small[49:50, :]
    put(dbuf, dw_hbm)
    put(kbuf, gain_hbm)
    for c_ in outs:
        c_.wait()


def finish(gin, small, big):
    vm, dma = pltpu.VMEM, pltpu.SemaphoreType.DMA
    any_, here = pl.BlockSpec(memory_space=pl.ANY), pl.BlockSpec(memory_space=pltpu.VMEM)
    n_ch = len(CHUNKS)
    gin, dw, gain, up, down = pl.pallas_call(
        finish_kernel,
        out_shape=(
            jax.ShapeDtypeStruct((PIX, CH), BF16),
            jax.ShapeDtypeStruct((49, CH), F32),
            jax.ShapeDtypeStruct((1, CH), F32),
            jax.ShapeDtypeStruct((CH, FF), F32),
            jax.ShapeDtypeStruct((FF, CH), F32),
        ),
        in_specs=[here] * (2 + 2 * n_ch),
        out_specs=[any_] * 5,
        scratch_shapes=[vm((49, CH), F32), vm((1, CH), F32)]
        + [vm((w, CH), F32) for w in CHUNKS]
        + [vm((CH, w), F32) for w in CHUNKS]
        + [dma((2 * n_ch + 3,))],
        compiler_params=pltpu.CompilerParams(vmem_limit_bytes=24_000_000),
        name="finish",
    )(gin, small, *[b.reshape(1024, w // 2) for b, w in zip(big, CHUNKS * 2)])
    return gin.reshape(ROWS, COLS, CH), dw, gain.reshape(CH), up, down


def on_device(features, dw_weight, norm_gain, w_up, w_down, cotangent):
    vm, dma = pltpu.VMEM, pltpu.SemaphoreType.DMA
    any_ = pl.BlockSpec(memory_space=pl.ANY)
    n_ch = len(CHUNKS)
    comm = []
    for c, w in enumerate(CHUNKS):
        h = w // 2
        whole = vm((4, 16, 16, h), BF16)
        comm += [vm((2, 1024, h), F32), whole, whole, whole]
        comm += [vm((2, 8, 16, h), BF16), vm((2, 16, 16, h), BF16), vm((3 if direct(c) else 2, 16, 16, h), BF16)]
        comm += [vm((16, 16, h), BF16), vm((15, 16, h), BF16)]
    gin, small, *big = pl.pallas_call(
        kernel,
        out_shape=(
            vm((PIX, CH), BF16),
            vm((64, CH), F32),
            *[vm((4, 16, 16, w // 2), BF16) for w in CHUNKS * 2],
        ),
        in_specs=[any_] * 6,
        out_specs=[pl.BlockSpec(memory_space=pltpu.VMEM)] * (2 + 2 * n_ch),
        scratch_shapes=[
            vm((ROWS, COLS, CH), BF16), vm((PIX, CH), BF16), vm((CH, FF), BF16), vm((FF, CH), BF16),
            vm((49, CH), F32), vm((1, CH), F32),
            vm((4, 14, 144, 128), F32), vm((4, 14, 144, 128), F32), vm((4, 49, 8, 128), F32),
            vm((4, PIX, 128), F32), vm((4, PIX, 128), F32), vm((PIX, 128), F32), vm((PIX, CH), BF16), vm((CH, PIX), BF16),
            vm((PIX, max(CHUNKS)), BF16), vm((PIX, FF), BF16), vm((PIX, CH), F32),
            vm((ROWS, COLS, CH), BF16),
            vm((2, 2, 8, 8, CH), BF16), vm((2, 2, 3, COLS, CH), BF16), vm((2, 2, 8, 8, CH), BF16), vm((2, 4, 3, 8, CH), BF16),
            vm((4, 64, 128), F32), vm((32, 8, 128), F32), vm((31, 8, 128), F32), vm((4, 8, 128), F32),
            vm((32, 8, 128), F32),
        ]
        + comm
        + [
            dma((6,)), dma((2, 8)), dma((2, 8)), dma((n_ch, 12)), dma((n_ch, 12)), dma((3,)), dma((3,)),
            pltpu.SemaphoreType.REGULAR((4,)),
        ],
        compiler_params=pltpu.CompilerParams(
            collective_id=0, has_side_effects=True, vmem_limit_bytes=58_000_000
        ),
        name="block_backward",
    )(features, dw_weight, norm_gain.reshape(1, CH), w_up, w_down, cotangent.reshape(PIX, CH))
    return finish(gin, small, big)


def solution(mesh):
    return jax.shard_map(
        on_device,
        mesh=mesh,
        in_specs=(P("rows", "cols", None), P(), P(), P(), P(), P("rows", "cols", None)),
        out_specs=(P("rows", "cols", None), P(), P(), P(), P()),
        check_vma=False,
    )
```

```python
import jax
import jax.numpy as jnp
from jax import lax
from jax.experimental import pallas as pl
from jax.experimental.pallas import tpu as pltpu
from jax.sharding import PartitionSpec as P

EPS = 1e-06
ROWS, COLS, CH, FF = 8, 128, 512, 2048
PIX = ROWS * COLS
CHUNKS = (512, 512, 512, 256, 256)
STARTS = tuple(sum(CHUNKS[:n]) for n in range(len(CHUNKS)))
LEFT = 8
F32, BF16 = jnp.float32, jnp.bfloat16
MESH = pl.DeviceIdType.MESH
FIRST_AXIS = ((0, 2), (1, 0), (2, 1), (0, 2), (2, 0))
SIDES = ((-1, 0), (1, 0), (0, -1), (0, 1), (-1, -1), (-1, 1), (1, -1), (1, 1))
(R_CORE, R_A0, R_A1, R_B0, R_B1, R_PRS, R_PAG, R_G0, R_G1, R_H0, R_H1, R_CAG) = range(12)


def direct(c):
    return c > 1


def kernel(*refs):
    refs = list(refs)

    def take(n):
        out = refs[:n]
        del refs[:n]
        return out

    feat_hbm, dww_hbm, gain_hbm, wup_hbm, wdn_hbm, cot_hbm = take(6)
    obuf, dout = take(2)
    GA, GB = take(len(CHUNKS)), take(len(CHUNKS))
    fbuf, cbuf, wup, wdn, dww, gainb, xf, gp, wb, cv, nv, invb, sc, sct = take(14)
    act, gh, gs, gb, scol, hrow, hcol, hcor = take(8)
    gd, dsm, dpr, dax, dga = take(5)
    G, csend, crecv, M, axa, axs, axb, pls, plr = zip(*[take(9) for _ in CHUNKS])
    ld, hsend, hrecv, csem, rsem, ssend, srecv, near = take(8)

    ra, ca = lax.axis_index("rows"), lax.axis_index("cols")
    core = ra % 2
    y, z, x = (ra // 2) % 4, ra // 8, ca

    def device(x_, y_, z_, core_):
        return ((z_ * 4 + y_) * 2 + core_, x_)

    partner = device(x, y, z, 1 - core)

    def side(dr, dc):
        return ((ra + dr + 32) % 32, (ca + dc + 4) % 4)

    def plane_peer(d, axis):
        ix, iy, iz = axis
        u, v = ix * y + iy * z + iz * x, ix * z + iy * x + iz * y
        u2, v2 = (u + d // 4) % 4, (v + d % 4) % 4
        return (
            device(
                ix * x + iy * v2 + iz * u2,
                ix * u2 + iy * y + iz * v2,
                ix * v2 + iy * u2 + iz * z,
                core,
            ),
            u2 * 4 + v2,
        )

    def plane_pos(axis):
        ix, iy, iz = axis
        return (ix * y + iy * z + iz * x) * 4 + ix * z + iy * x + iz * y

    def pair_peer(d):
        x2, y2, core2 = (x + d // 8) % 4, (y + (d // 2) % 4) % 4, (core + d % 2) % 2
        return device(x2, y2, z, core2), (x2 * 4 + y2) * 2 + core2

    def axis_of(c):
        a0, a1 = FIRST_AXIS[c]
        return tuple((a0 == n) * (1 - core) + (a1 == n) * core for n in range(3))

    def along(axis, step):
        ix, iy, iz = axis
        return device(
            (x + step * ix) % 4, (y + step * iy) % 4, (z + step * iz) % 4, core
        )

    def remote(src, dst, send, recv, to):
        return pltpu.make_async_remote_copy(
            src_ref=src, dst_ref=dst, send_sem=send, recv_sem=recv, device_id=to, device_id_type=MESH
        )

    def landed(ref, sem):
        pltpu.make_async_copy(ref, ref, sem).wait()

    loads = [
        pltpu.make_async_copy(s, d, ld.at[n])
        for n, (s, d) in enumerate(
            ((feat_hbm, fbuf), (dww_hbm, dww), (gain_hbm, gainb), (cot_hbm, cbuf), (wup_hbm, wup), (wdn_hbm, wdn))
        )
    ]
    for c_ in loads:
        c_.start()
    barrier = pltpu.get_barrier_semaphore()
    for dr, dc in SIDES:
        pl.semaphore_signal(barrier, inc=1, device_id=side(dr, dc), device_id_type=MESH)

    NEAR = [along(tuple(int(n == k) for n in range(3)), step) for k in range(3) for step in (1, 3)]
    for to in NEAR:
        pl.semaphore_signal(barrier, inc=1, device_id=to, device_id_type=MESH)

    def round_signal(n):
        for to in [partner] + NEAR:
            pl.semaphore_signal(near.at[n], inc=1, device_id=to, device_id_type=MESH)

    def round_wait(n):
        pl.semaphore_wait(near.at[n], 1 + len(NEAR))

    for c_ in loads[:3]:
        c_.wait()

    def edges(pad, phase):
        for n, start in ((0, LEFT), (1, LEFT + COLS - 8)):
            for cc in range(4):
                scol[phase, n, :, :, cc * 128 : cc * 128 + 128] = pad[
                    cc, 3 : 3 + ROWS, start : start + 8, :
                ].astype(BF16)

    with jax.named_scope("widen"):
        @pl.loop(0, ROWS)
        def _(r):
            for cc in range(4):
                xf[cc, 3 + r, LEFT : LEFT + COLS, :] = fbuf[r, :, cc * 128 : cc * 128 + 128].astype(F32)

        edges(xf, 0)
        for cc in range(4):
            gd[cc, 48:64, :] = jnp.zeros((16, 128), F32)

    with jax.named_scope("entry"):
        pl.semaphore_wait(barrier, len(SIDES) + len(NEAR))
        round_signal(0)

    def halo_copies(phase, rows_src):
        out = []
        for n, (dr, dc) in enumerate(SIDES):
            rs = slice(0, 3) if dr < 0 else slice(5, 8)
            if dc == 0:
                src, dst = rows_src.at[rs], hrow.at[phase, n]
            elif dr == 0:
                src, dst = scol.at[phase, n - 2], hcol.at[phase, n - 2]
            else:
                src, dst = scol.at[phase, 0 if dc < 0 else 1, rs], hcor.at[phase, n - 4]
            if dc == 0 and phase == 1:
                cols = [pl.ds(32 * k, 32) for k in range(4)]
                out.append([
                    remote(src.at[:, k], dst.at[:, k], hsend.at[1, n], hrecv.at[1, n], side(dr, dc)) for k in cols
                ])
            else:
                out.append([remote(src, dst, hsend.at[phase, n], hrecv.at[phase, n], side(dr, dc))])
        return out

    def halo_landed(phase, n):
        buf = hrow.at[phase, n] if n < 2 else hcol.at[phase, n - 2] if n < 4 else hcor.at[phase, n - 4]
        landed(buf, hrecv.at[phase, n])

    valid = {
        -1: jnp.where(ra < 31, 1.0, 0.0).astype(F32),
        1: jnp.where(ra > 0, 1.0, 0.0).astype(F32),
    }
    valid_c = {
        -1: jnp.where(ca < 3, 1.0, 0.0).astype(F32),
        1: jnp.where(ca > 0, 1.0, 0.0).astype(F32),
    }

    def halo_cols(phase, pad):
        for n in (2, 3):
            halo_landed(phase, n)
            dc = SIDES[n][1]
            start = LEFT + COLS if dc < 0 else LEFT - 8
            for cc in range(4):
                pad[cc, 3 : 3 + ROWS, start : start + 8, :] = (
                    hcol[phase, n - 2, :, :, cc * 128 : cc * 128 + 128].astype(F32) * valid_c[dc]
                )

    def halo_rows(phase, pad):
        for n in (0, 1):
            halo_landed(phase, n)
            dr = SIDES[n][0]
            r0 = 3 + ROWS if dr < 0 else 0
            for r in range(3):
                for cc in range(4):
                    pad[cc, r0 + r, LEFT : LEFT + COLS, :] = (
                        hrow[phase, n, r, :, cc * 128 : cc * 128 + 128].astype(F32) * valid[dr]
                    )
        for n in range(4, 8):
            halo_landed(phase, n)
            dr, dc = SIDES[n]
            r0 = 3 + ROWS if dr < 0 else 0
            start = LEFT + COLS if dc < 0 else LEFT - 8
            for cc in range(4):
                pad[cc, r0 : r0 + 3, start : start + 8, :] = hcor[
                    phase, n - 4, :, :, cc * 128 : cc * 128 + 128
                ].astype(F32) * (valid[dr] * valid_c[dc])

    def conv(pad, flip, cc, starts, inner):
        rhos = range(3, 11) if inner else (0, 1, 2, 11, 12, 13)
        rows = range(ROWS) if inner else (0, 1, 2, 5, 6, 7)

        def at(r, b):
            return pl.ds(pl.multiple_of(r * COLS + starts[b], 8), 8)

        def body(j, acc):
            acc = dict(zip([(r, b) for r in rows for b in range(4)], acc))
            w = [wb[cc, (48 - 7 * i - j) if flip else (7 * i + j)] for i in range(7)]
            for rho in rhos:
                for b in range(4):
                    v = pad[cc, rho, pl.ds(starts[b] + (LEFT - 3) + j, 8), :]
                    for r in rows:
                        if 0 <= rho - r <= 6:
                            acc[r, b] = acc[r, b] + v * w[rho - r]
            return tuple(acc.values())

        if inner:
            start = tuple(jnp.zeros((8, 128), F32) for r in rows for b in range(4))
        else:
            start = tuple(cv[cc, at(r, b), :] for r in rows for b in range(4))
        acc = lax.fori_loop(0, 7, body, start, unroll=7)
        for n, (r, b) in enumerate([(r, b) for r in rows for b in range(4)]):
            cv[cc, at(r, b), :] = acc[n]

    def groups(base):
        return [base + 8 * b for b in range(4)]

    halo = halo_copies(0, fbuf)
    with jax.named_scope("taps"):
        for n in (2, 3, 0, 1, 4, 5, 6, 7):
            halo[n][0].start()

        for t in range(49):
            for cc in range(4):
                wb[cc, t] = jnp.broadcast_to(dww[t : t + 1, cc * 128 : cc * 128 + 128], (8, 128))

    with jax.named_scope("fconv_mid"):
        @pl.loop(0, 12)
        def _(t):
            conv(xf, False, t // 3, groups(8 + 32 * (t % 3)), True)

    with jax.named_scope("fhalo_c"):
        round_wait(0)
        round_signal(1)
        halo_cols(0, xf)

    with jax.named_scope("fconv_side"):
        @pl.loop(0, 4)
        def _(t):
            conv(xf, False, t, (0, 104, 112, 120), True)

    with jax.named_scope("fhalo_r"):
        round_wait(1)
        round_signal(2)
        halo_rows(0, xf)

    with jax.named_scope("fconv_out"):
        @pl.loop(0, 16)
        def _(t):
            conv(xf, False, t // 4, groups(32 * (t % 4)), False)

    round_wait(2)
    round_signal(3)

    def norm(quarter):
        for t in range(4):
            ps = slice(quarter * 256 + t * 64, quarter * 256 + t * 64 + 64)
            v = [cv[cc, ps, :] for cc in range(4)]
            mean = jnp.sum(v[0] + v[1] + v[2] + v[3], axis=1, keepdims=True) * (1.0 / CH)
            v = [a - mean for a in v]
            sq = [a * a for a in v]
            inv = lax.rsqrt(jnp.sum(sq[0] + sq[1] + sq[2] + sq[3], axis=1, keepdims=True) * (1.0 / CH) + EPS)
            invb[ps, :] = jnp.broadcast_to(inv, (64, 128))
            for cc in range(4):
                n_ = v[cc] * inv
                nv[cc, ps, :] = n_
                sc[ps, cc * 128 : cc * 128 + 128] = (n_ * gainb[:, cc * 128 : cc * 128 + 128]).astype(BF16)

    for c_ in loads[3:]:
        c_.wait()

    def last_round():
        round_wait(3)

    def mlp_a(c, pbs):
        w = CHUNKS[c]
        fs = slice(STARTS[c], STARTS[c] + w)
        for pb in pbs:
            ps = slice(pb * 256, pb * 256 + 256)
            h = jnp.dot(sc[ps, :], wup[:, fs], preferred_element_type=F32)
            ga = lax.dot_general(cbuf[ps, :], wdn[fs, :], (((1,), (1,)), ((), ())), preferred_element_type=F32)
            phi = 0.5 * (1.0 + lax.erf(h * 0.7071067811865476))
            act[ps, 0:w] = (h * phi).astype(BF16)
            e = jnp.exp(-0.5 * h * h) * 0.3989422804014327
            gh[ps, fs] = (ga * (phi + h * e)).astype(BF16)

    def put(c, slot, value):
        w, rows = CHUNKS[c] // 2, value.shape[0]
        for n in range(1024 // rows):
            G[c][slot, n * rows : (n + 1) * rows, :] = value[:, n * w : (n + 1) * w]

    def mlp_down(c):
        put(c, core, lax.dot_general(
            act[:, 0 : CHUNKS[c]], cbuf[...], (((0,), (0,)), ((), ())), preferred_element_type=F32))

    def mlp_up(c):
        fs = slice(STARTS[c], STARTS[c] + CHUNKS[c])
        if CHUNKS[c] < 512:
            for n in range(2):
                rs = slice(n * 256, n * 256 + 256)
                v = jnp.dot(sct[rs, :], gh[:, fs], preferred_element_type=F32)
                w = CHUNKS[c] // 2
                for k in range(2):
                    G[c][1 - core, k * 512 + n * 256 : k * 512 + n * 256 + 256, :] = v[:, k * w : (k + 1) * w]
        else:
            put(c, 1 - core, jnp.dot(sct[...], gh[:, fs], preferred_element_type=F32))

    def mlp_back(q):
        ps = slice(q * 256, q * 256 + 256)
        gs[ps, :] = lax.dot_general(gh[ps, :], wup[...], (((1,), (1,)), ((), ())), preferred_element_type=F32)

    def blocks(fn):
        @pl.loop(0, 8)
        def _(t):
            fn(t // 2, pl.ds((t % 2) * 8, 8), pl.ds(pl.multiple_of(t * 128, 128), 128))

    def place(c):
        axis = axis_of(c)
        return axis, axis[0] * x + axis[1] * y + axis[2] * z

    def send(c, n, src, dst, to):
        remote(src, dst, csem.at[c, n], rsem.at[c, n], to).start()

    def arrived(c, n, ref):
        landed(ref, rsem.at[c, n])

    def ch_core(c):
        def go(a, n, rows):
            csend[c][a, n] = G[c][1, rows, :].reshape(8, 16, CHUNKS[c] // 2).astype(BF16)
        blocks(go)
        send(c, R_CORE, csend[c], crecv[c], partner)

    def ch_axis(c):
        arrived(c, R_CORE, crecv[c])
        axis, p = place(c)
        def go(a, n, rows):
            M[c][a, n] = (
                G[c][0, rows, :].reshape(8, 16, CHUNKS[c] // 2) + crecv[c][a, n].astype(F32)
            ).astype(BF16)
        blocks(go)
        if direct(c):
            for d in (2, 1, 3):
                send(c, R_A0, M[c].at[(p + d) % 4], axb[c].at[d - 1], along(axis, d))
        else:
            far = (p + 2) % 4
            send(c, R_A0, M[c].at[far, 0:8], axa[c].at[0], along(axis, 1))
            send(c, R_A1, M[c].at[far, 8:16], axa[c].at[1], along(axis, 3))

    def ch_axis2(c):
        axis, p = place(c)
        arrived(c, R_A0, axa[c].at[0])
        arrived(c, R_A1, axa[c].at[1])
        right, left = (p + 1) % 4, (p + 3) % 4
        axs[c][0, 0:8] = (M[c][right, 0:8].astype(F32) + axa[c][0].astype(F32)).astype(BF16)
        axs[c][0, 8:16] = M[c][right, 8:16]
        send(c, R_B0, axs[c].at[0], axb[c].at[0], along(axis, 1))
        axs[c][1, 0:8] = M[c][left, 0:8]
        axs[c][1, 8:16] = (M[c][left, 8:16].astype(F32) + axa[c][1].astype(F32)).astype(BF16)
        send(c, R_B1, axs[c].at[1], axb[c].at[1], along(axis, 3))

    def ch_plane(c):
        axis, p = place(c)
        if direct(c):
            arrived(c, R_A0, axb[c])
        else:
            arrived(c, R_B0, axb[c].at[0])
            arrived(c, R_B1, axb[c].at[1])
        total = M[c][p].astype(F32)
        for n in range(3 if direct(c) else 2):
            total = total + axb[c][n].astype(F32)
        pls[c][...] = total.astype(BF16)

        @pl.loop(1, 16, unroll=15)
        def _(d):
            to, pos = plane_peer(d, axis)
            send(c, R_PRS, pls[c].at[pos], plr[c].at[d - 1], to)

    def ch_share(c):
        axis, p = place(c)
        pos = plane_pos(axis)
        arrived(c, R_PRS, plr[c])
        total = pls[c][pos].astype(F32)
        for d in range(15):
            total = total + plr[c][d].astype(F32)
        GA[c][p, pos] = total.astype(BF16)

        @pl.loop(1, 16, unroll=15)
        def _(d):
            to, _ = plane_peer(d, axis)
            send(c, R_PAG, GA[c].at[p, pos], GA[c].at[p, pos], to)

    def ch_back(c):
        axis, p = place(c)
        arrived(c, R_PAG, plr[c])
        if direct(c):
            for d in (2, 1, 3):
                send(c, R_G0, GA[c].at[p], GA[c].at[p], along(axis, d))
        else:
            send(c, R_G0, GA[c].at[p], GA[c].at[p], along(axis, 1))
            send(c, R_G1, GA[c].at[p], GA[c].at[p], along(axis, 3))
        send(c, R_CAG, GA[c].at[p], GB[c].at[p], partner)

    def ch_back2(c):
        axis, p = place(c)
        right, left = (p + 1) % 4, (p + 3) % 4
        arrived(c, R_G0, GA[c].at[left])
        arrived(c, R_G1, GA[c].at[right])
        a, b = GA[c].at[left, 0:8], GA[c].at[right, 8:16]
        send(c, R_H0, a, a, along(axis, 1))
        send(c, R_H1, b, b, along(axis, 3))
        for q in (left, right):
            send(c, R_CAG, GA[c].at[q], GB[c].at[q], partner)

    def ch_pair(c):
        axis, p = place(c)
        if direct(c):
            arrived(c, R_G0, axb[c])
            for d in (1, 2, 3):
                q = (p + d) % 4
                send(c, R_CAG, GA[c].at[q], GB[c].at[q], partner)
        else:
            arrived(c, R_H0, axa[c].at[0])
            arrived(c, R_H1, axa[c].at[1])
            far = (p + 2) % 4
            send(c, R_CAG, GA[c].at[far], GB[c].at[far], partner)

    def ch_end(c):
        arrived(c, R_CAG, GB[c])

    def ln_back(quarter):
        def body(t, part):
            ps = slice(quarter * 256 + t * 64, quarter * 256 + t * 64 + 64)
            inv = invb[ps, :]
            ns = [nv[cc, ps, :] for cc in range(4)]
            gv = [gs[ps, cc * 128 : cc * 128 + 128] for cc in range(4)]
            prod = [g * n for g, n in zip(gv, ns)]
            part = tuple(
                q + jnp.sum(pr.reshape(8, 8, 128), axis=0) for q, pr in zip(part, prod)
            )
            gains = [gainb[:, cc * 128 : cc * 128 + 128] for cc in range(4)]
            gn = [g * k for g, k in zip(gv, gains)]
            gm = [pr * k for pr, k in zip(prod, gains)]
            m1 = jnp.sum(gn[0] + gn[1] + gn[2] + gn[3], axis=1, keepdims=True) * (1.0 / CH)
            m2 = jnp.sum(gm[0] + gm[1] + gm[2] + gm[3], axis=1, keepdims=True) * (1.0 / CH)
            r, c0 = 2 * quarter + t // 2, (t % 2) * 64
            for cc in range(4):
                g = (inv * (gn[cc] - m1 - ns[cc] * m2)).astype(BF16)
                gb[r, c0 : c0 + 64, cc * 128 : cc * 128 + 128] = g
                gp[cc, 3 + r, LEFT + c0 : LEFT + c0 + 64, :] = g.astype(F32)
            return part

        part = tuple(jnp.zeros((8, 128), F32) for _ in range(4))
        for t in range(4):
            part = body(t, part)
        for cc in range(4):
            row = jnp.sum(part[cc], axis=0, keepdims=True)
            gd[cc, 49:50, :] = row if quarter == 0 else gd[cc, 49:50, :] + row

    back = halo_copies(1, gb)

    def send_back():
        edges(gp, 1)
        for n in (2, 3, 4, 5, 6, 7):
            back[n][0].start()

    def send_rows(k):
        back[0][k].start()
        back[1][k].start()

    def gdw(cc, js):
        @pl.loop(js[0], js[1])
        def _(j):
            def body(cb, acc):
                acc = list(acc)
                base = cb * 64
                for b in range(8):
                    gv = [gp[cc, 3 + r, pl.ds(pl.multiple_of(base + LEFT + 8 * b, 8), 8), :] for r in range(8)]
                    for rho in range(14):
                        v = xf[cc, rho, pl.ds(base + (8 * b + LEFT - 3) + j, 8), :]
                        for r in range(max(0, rho - 6), min(8, rho + 1)):
                            acc[rho - r] = acc[rho - r] + v * gv[r]
                return tuple(acc)

            acc = lax.fori_loop(0, 2, body, tuple(jnp.zeros((8, 128), F32) for _ in range(7)))
            for i in range(7):
                gd[cc, pl.ds(7 * i + j, 1), :] = jnp.sum(acc[i], axis=0, keepdims=True)

    zaxis = (0, 0, 1)
    mine = (x * 4 + y) * 2 + core

    def sm_scatter():
        for cc in range(4):
            for tb in range(8):
                dsm[8 * cc + tb] = gd[cc, 8 * tb : 8 * tb + 8, :]

        @pl.loop(1, 32, unroll=31)
        def _(d):
            to, pos = pair_peer(d)
            remote(dsm.at[pos], dpr.at[d - 1], ssend.at[0], srecv.at[0], to).start()

    def sm_axis():
        landed(dpr, srecv.at[0])
        total = dsm[mine]
        for d in range(31):
            total = total + dpr[d]
        dax[z] = total
        for step in (2, 1, 3):
            remote(dax.at[z], dax.at[z], ssend.at[1], srecv.at[1], along(zaxis, step)).start()

    def sm_share():
        landed(dpr.at[0:3], srecv.at[1])
        dga[mine] = dax[0] + dax[1] + dax[2] + dax[3]

        @pl.loop(1, 32, unroll=31)
        def _(d):
            to, _ = pair_peer(d)
            remote(dga.at[mine], dga.at[mine], ssend.at[2], srecv.at[2], to).start()

    def sm_end():
        landed(dpr, srecv.at[2])
        for cc in range(4):
            for tb in range(8):
                dout[8 * tb : 8 * tb + 8, cc * 128 : cc * 128 + 128] = dga[8 * cc + tb]

    def gin_inner(cb, half):
        @pl.loop(2 * half, 2 * half + 2)
        def _(t):
            conv(gp, True, t, groups(32 * cb), True)

    def gin_outer(cb):
        @pl.loop(0, 4)
        def _(t):
            conv(gp, True, t, groups(32 * cb), False)

    def gin_store(part):
        @pl.loop(part * 8, part * 8 + 8)
        def _(t):
            ps = pl.ds(pl.multiple_of(t * 64, 64), 64)
            for cc in range(4):
                cs = slice(cc * 128, cc * 128 + 128)
                obuf[ps, cs] = (cbuf[ps, cs].astype(F32) + cv[cc, ps, :]).astype(BF16)

    def norm_a():
        for q in range(5):
            if q < 4:
                norm(q)
                qs = slice(q * 256, q * 256 + 256)
                sct[:, qs] = sc[qs, :].T
            if q > 0:
                mlp_a(0, (q - 1,))

    work = []
    chains = {}
    for c, w in enumerate(CHUNKS):
        k = w / 512
        if c == 0:
            work += [(3.0, "norm_a", norm_a, None)]
        else:
            work += [(0.75 * k, "mlp_a", lambda c=c, p=p: mlp_a(c, p), None) for p in ((0, 1), (2, 3))]
        if c == 1:
            work += [(0.01, "last_round", last_round, None)]
        work += [(0.73 * k, "mlp_down", lambda c=c: mlp_down(c), None), (0.73 * k, "mlp_up", lambda c=c: mlp_up(c), c)]
        if direct(c):
            steps = (
                (0.0, ch_core), (2.2, ch_axis), (5.0 + 2.0 * k, ch_plane), (7.0, ch_share), (6.0, ch_back), (6.0, ch_pair), (2.5, ch_end)
            )
        else:
            steps = (
                (0.0, ch_core), (2.5, ch_axis), (4.0, ch_axis2), (5.0, ch_plane), (7.0, ch_share),
                (6.0, ch_back), (5.0, ch_back2), (5.0, ch_pair), (2.5, ch_end),
            )
        more = {(2, ch_back): 1.8}
        steps = tuple((gap + more.get((c, fn), 0.0), fn) for gap, fn in steps)
        chains[c] = [((0.85 if n < 4 else 0.85) * gap, fn.__name__, lambda fn=fn, c=c: fn(c)) for n, (gap, fn) in enumerate(steps)]
    def both(q):
        if q < 4:
            mlp_back(q)
        if q > 0:
            ln_back(q - 1)

    work += [(0.73, "back", lambda q=q: both(q), None) for q in range(5)]
    work += [(0.1, "send_back", send_back, None)]
    small = len(CHUNKS)
    for cc in range(4):
        work += [(0.8, "gdw", lambda cc=cc: gdw(cc, (0, 3)), None)]
        work += [(0.02, "send_rows", lambda cc=cc: send_rows(cc), None)]
        work += [(0.55, "gdw", lambda cc=cc: gdw(cc, (3, 5)), None)]
        work += [(0.55, "gdw", lambda cc=cc: gdw(cc, (5, 7)), small if cc == 3 else None)]
    steps = ((0.0, sm_scatter), (4.6, sm_axis), (3.6, sm_share), (6.0, sm_end))
    chains[small] = [(gap, fn.__name__, fn) for gap, fn in steps]
    for n, cb in enumerate((1, 2, 0, 3)):
        if n == 2:
            work += [(0.05, "halo_c", lambda: halo_cols(1, gp), None)]
        work += [(0.85, "gin_in", lambda cb=cb, half=half: gin_inner(cb, half), None) for half in (0, 1)]
    work += [(0.15, "halo_r", lambda: halo_rows(1, gp), None)]
    work += [(0.7, "gin_out", lambda cb=cb: gin_outer(cb), None) for cb in range(4)]
    work += [(0.2, "gin_st", lambda: gin_store(0), None), (0.2, "gin_st", lambda: gin_store(1), None)]

    now = 0.0
    due = []

    def serve(limit):
        nonlocal now
        while due and (limit is None or min(due)[0] <= limit):
            when, key, n = min(due)
            due.remove((when, key, n))
            now = max(now, when) + 0.1
            with jax.named_scope(f"{chains[key][n][1]}_{key}"):
                chains[key][n][2]()
            if n + 1 < len(chains[key]):
                due.append((now + chains[key][n + 1][0], key, n + 1))

    def drain(chunks, steps):
        for c in chunks:
            sent = [(R_CORE, csend[c]), (R_PRS, plr[c]), (R_PAG, plr[c]), (R_CAG, GA[c])]
            if direct(c):
                sent += [(R_A0, axb[c]), (R_G0, axb[c])]
            else:
                sent += [(R_A0, axa[c].at[0]), (R_A1, axa[c].at[1]), (R_B0, axb[c].at[0]), (R_B1, axb[c].at[1])]
                sent += [(R_G0, axb[c].at[0]), (R_G1, axb[c].at[1]), (R_H0, axa[c].at[0]), (R_H1, axa[c].at[1])]
            for n, ref in sent:
                if n in steps:
                    landed(ref, csem.at[c, n])

    def early_drain():
        for phase in (0, 1):
            for n in range(8):
                buf = hrow.at[phase, n] if n < 2 else hcol.at[phase, n - 2] if n < 4 else hcor.at[phase, n - 4]
                landed(buf, hsend.at[phase, n])
        drain(range(len(CHUNKS)), (R_CORE, R_A0, R_A1, R_B0, R_B1, R_PRS, R_PAG))
        landed(dpr, ssend.at[0])
        landed(dpr.at[0:3], ssend.at[1])

    for cost, name, fn, opens in work:
        with jax.named_scope(name):
            fn()
        now += cost
        if opens is not None:
            due.append((now, opens, 0))
        serve(now)
    with jax.named_scope("early"):
        early_drain()
    serve(None)

    with jax.named_scope("drain"):
        drain(range(len(CHUNKS)), (R_G0, R_G1, R_H0, R_H1, R_CAG))
        landed(dpr, ssend.at[2])


def finish_kernel(*refs):
    refs = list(refs)
    n_ch = len(CHUNKS)
    gin, small = refs[:2]
    own, other = refs[2 : 2 + n_ch], refs[2 + n_ch : 2 + 2 * n_ch]
    gout_hbm, dw_hbm, gain_hbm, up_hbm, down_hbm, dbuf, kbuf = refs[2 + 2 * n_ch : 9 + 2 * n_ch]
    downs, ups = refs[9 + 2 * n_ch : 9 + 3 * n_ch], refs[9 + 3 * n_ch : 9 + 4 * n_ch]
    osem = refs[-1]
    outs = []

    def put(src, dst):
        outs.append(pltpu.make_async_copy(src, dst, osem.at[len(outs)]))
        outs[-1].start()

    def widen(c, down, up):
        half = CHUNKS[c] // 2
        for narrow, wide in ((down, downs[c]), (up, ups[c])):
            rows = wide.shape[0]
            step = rows // 4

            @pl.loop(0, 4)
            def _(t):
                rs = pl.ds(pl.multiple_of(t * step, step), step)
                for n in range(1024 // rows):
                    wide[rs, n * half : (n + 1) * half] = narrow[
                        pl.ds(pl.multiple_of(n * rows + t * step, step), step), :
                    ].astype(F32)

    put(gin, gout_hbm)
    dbuf[...] = small[0:49, :]
    kbuf[...] = small[49:50, :]
    put(dbuf, dw_hbm)
    put(kbuf, gain_hbm)
    core = lax.axis_index("rows") % 2
    for c, w in enumerate(CHUNKS):
        @pl.when(core == 0)
        def _():
            widen(c, own[c], other[c])

        @pl.when(core == 1)
        def _():
            widen(c, other[c], own[c])

        part = pl.ds(STARTS[c], w)
        put(downs[c], down_hbm.at[part])
        put(ups[c], up_hbm.at[:, part])
    for c_ in outs:
        c_.wait()


def finish(gin, small, big):
    vm, dma = pltpu.VMEM, pltpu.SemaphoreType.DMA
    any_, here = pl.BlockSpec(memory_space=pl.ANY), pl.BlockSpec(memory_space=pltpu.VMEM)
    n_ch = len(CHUNKS)
    gin, dw, gain, up, down = pl.pallas_call(
        finish_kernel,
        out_shape=(
            jax.ShapeDtypeStruct((PIX, CH), BF16),
            jax.ShapeDtypeStruct((49, CH), F32),
            jax.ShapeDtypeStruct((1, CH), F32),
            jax.ShapeDtypeStruct((CH, FF), F32),
            jax.ShapeDtypeStruct((FF, CH), F32),
        ),
        in_specs=[here] * (2 + 2 * n_ch),
        out_specs=[any_] * 5,
        scratch_shapes=[vm((49, CH), F32), vm((1, CH), F32)]
        + [vm((w, CH), F32) for w in CHUNKS]
        + [vm((CH, w), F32) for w in CHUNKS]
        + [dma((2 * n_ch + 3,))],
        compiler_params=pltpu.CompilerParams(vmem_limit_bytes=24_000_000),
        name="finish",
    )(gin, small, *[b.reshape(1024, w // 2) for b, w in zip(big, CHUNKS * 2)])
    return gin.reshape(ROWS, COLS, CH), dw, gain.reshape(CH), up, down


def on_device(features, dw_weight, norm_gain, w_up, w_down, cotangent):
    vm, dma = pltpu.VMEM, pltpu.SemaphoreType.DMA
    any_ = pl.BlockSpec(memory_space=pl.ANY)
    n_ch = len(CHUNKS)
    comm = []
    for c, w in enumerate(CHUNKS):
        h = w // 2
        whole = vm((4, 16, 16, h), BF16)
        comm += [vm((2, 1024, h), F32), whole, whole, whole]
        comm += [vm((2, 8, 16, h), BF16), vm((2, 16, 16, h), BF16), vm((3 if direct(c) else 2, 16, 16, h), BF16)]
        comm += [vm((16, 16, h), BF16), vm((15, 16, h), BF16)]
    gin, small, *big = pl.pallas_call(
        kernel,
        out_shape=(
            vm((PIX, CH), BF16),
            vm((64, CH), F32),
            *[vm((4, 16, 16, w // 2), BF16) for w in CHUNKS * 2],
        ),
        in_specs=[any_] * 6,
        out_specs=[pl.BlockSpec(memory_space=pltpu.VMEM)] * (2 + 2 * n_ch),
        scratch_shapes=[
            vm((ROWS, COLS, CH), BF16), vm((PIX, CH), BF16), vm((CH, FF), BF16), vm((FF, CH), BF16),
            vm((49, CH), F32), vm((1, CH), F32),
            vm((4, 14, 144, 128), F32), vm((4, 14, 144, 128), F32), vm((4, 49, 8, 128), F32),
            vm((4, PIX, 128), F32), vm((4, PIX, 128), F32), vm((PIX, 128), F32), vm((PIX, CH), BF16), vm((CH, PIX), BF16),
            vm((PIX, max(CHUNKS)), BF16), vm((PIX, FF), BF16), vm((PIX, CH), F32),
            vm((ROWS, COLS, CH), BF16),
            vm((2, 2, 8, 8, CH), BF16), vm((2, 2, 3, COLS, CH), BF16), vm((2, 2, 8, 8, CH), BF16), vm((2, 4, 3, 8, CH), BF16),
            vm((4, 64, 128), F32), vm((32, 8, 128), F32), vm((31, 8, 128), F32), vm((4, 8, 128), F32),
            vm((32, 8, 128), F32),
        ]
        + comm
        + [
            dma((6,)), dma((2, 8)), dma((2, 8)), dma((n_ch, 12)), dma((n_ch, 12)), dma((3,)), dma((3,)),
            pltpu.SemaphoreType.REGULAR((4,)),
        ],
        compiler_params=pltpu.CompilerParams(
            collective_id=0, has_side_effects=True, vmem_limit_bytes=58_000_000
        ),
        name="block_backward",
    )(features, dw_weight, norm_gain.reshape(1, CH), w_up, w_down, cotangent.reshape(PIX, CH))
    return finish(gin, small, big)


def solution(mesh):
    return jax.shard_map(
        on_device,
        mesh=mesh,
        in_specs=(P("rows", "cols", None), P(), P(), P(), P(), P("rows", "cols", None)),
        out_specs=(P("rows", "cols", None), P(), P(), P(), P()),
        check_vma=False,
    )
```
